32 devices in a mesh: curve: 8 (over z, y), sub: 4 (over x, core).
Axes of the slice: x: 2, y: 2, z: 4, core: 2. Of those that a mesh axis runs over, the one named last changes fastest.
Arguments:
- forcing: float32 [12, 768, 1024], P(None, 'curve', 'sub'), may hold values from -10 to 10
- metric: float32 [768, 1024], P('curve', 'sub'), may hold values from 0.25 to 4
- jacobian: float32 [768, 1024], P('curve', 'sub'), may hold values from 0.5 to 2
- mode_scale: float32 [12], replicated, may hold values from 0.1 to 10
Outputs:
- solution: float32 [12, 768, 1024], P(None, 'curve', 'sub')
- residual: float32 [12, 768, 1024], P(None, 'curve', 'sub')
The draws below stay inside these ranges and needn't reach their ends.
All inputs are finite; a program needn't handle non-finite values.
Results may differ from the reference program's by a relative error of at most 0.0003.
Values sent between devices are 32-bit elements; how exact they have to be, the bound alone decides.
A program may use at most 64 MiB of HBM per device.

```python
import math
import jax
import jax.numpy as jnp
import numpy as np
from jax import lax

NP = 4
MODES = 12
ITERS = 3
EBX = 24
NX = 768
NY = 1024


def draw_forcing(key, part):
    noise_key, scale_key = jax.random.split(jax.random.fold_in(key, 7))
    regions = NX // (NP * EBX)
    region_scale = jnp.exp(jax.random.uniform(scale_key, (regions,), jnp.float32, math.log(0.3), math.log(3.0)))
    per_row = jnp.repeat(region_scale, NP * EBX)
    base = jax.random.normal(noise_key, (MODES, NX, NY), jnp.float32)
    return jnp.clip(base * per_row[None, :, None], -10.0, 10.0)


def block_scale(key, extent, cuts, low, high):
    level, own = 1.0, jax.random.fold_in(key, 6)
    for axis_at, blocks in cuts:
        steps = jnp.exp(jax.random.uniform(jax.random.fold_in(own, axis_at), (blocks,), jnp.float32, low / len(cuts), high / len(cuts)))
        level = level * jnp.repeat(steps, extent[axis_at] // blocks).reshape([-1 if axis == axis_at else 1 for axis in range(len(extent))])
    return level


def setup_inputs(seed: int = 0) -> dict:
    key_list = jax.random.split(jax.random.key(seed), 5)
    forcing = draw_forcing(jax.random.fold_in(key_list[4], 71), 0)
    metric = jnp.clip(jnp.exp(math.log(4.0) - 2.7725887 * jax.random.uniform(key_list[1], (NX, NY), jnp.float32) ** block_scale(key_list[1], (NX, NY), ((0, 8), (1, 4)), -0.2, 0.2)), 0.25, 4.0)
    jacobian = jnp.clip(jnp.exp(math.log(2.0) - 1.3862944 * jax.random.uniform(key_list[2], (NX, NY), jnp.float32) ** block_scale(key_list[2], (NX, NY), ((0, 8), (1, 4)), -0.2, 0.2)), 0.5, 2.0)
    mode_scale = jnp.clip(jnp.exp(jax.random.uniform(key_list[3], (MODES,), jnp.float32, math.log(0.1), math.log(10.0))), 0.1, 10.0)
    return {"forcing": forcing, "metric": metric, "jacobian": jacobian, "mode_scale": mode_scale}


def gll_tables():
    points = np.array([-1.0, -1.0 / math.sqrt(5.0), 1.0 / math.sqrt(5.0), 1.0])
    weights = np.array([1.0 / 6.0, 5.0 / 6.0, 5.0 / 6.0, 1.0 / 6.0])
    factor = np.array([np.prod([points[j] - points[m] for m in range(4) if m != j]) for j in range(4)])
    slopes = np.zeros((4, 4))
    for i in range(4):
        for j in range(4):
            if i != j:
                slopes[i, j] = factor[i] / (factor[j] * (points[i] - points[j]))
        slopes[i, i] = sum((1.0 / (points[i] - points[m]) for m in range(4) if m != i))
    return (slopes, weights)

def line_tables(count):
    phase = jnp.arange(count, dtype=jnp.int32) % 4
    on_edge = (phase == 0) | (phase == 3)
    line_w = jnp.where(on_edge, jnp.float32(1.0 / 6.0), jnp.float32(5.0 / 6.0))
    line_mult = jnp.where(on_edge, jnp.float32(2.0), jnp.float32(1.0))
    return (line_w, line_mult)

def assemble(values):
    for axis_dim in (0, 1):
        phase = lax.broadcasted_iota(jnp.int32, values.shape, axis_dim) % 4
        values = values + jnp.where(phase == 3, jnp.roll(values, -1, axis_dim), 0.0) + jnp.where(phase == 0, jnp.roll(values, 1, axis_dim), 0.0)
    return values

def apply_local(values, scale, slopes, mass_w, flux_w):
    row_count, col_count = values.shape
    shape4 = (row_count // 4, 4, col_count // 4, 4)
    blocks = values.reshape(shape4)
    hp = lax.Precision.HIGHEST
    grad_x = jnp.einsum('ak,xkyb->xayb', slopes, blocks, precision=hp)
    grad_y = jnp.einsum('bk,xayk->xayb', slopes, blocks, precision=hp)
    weight4 = flux_w.reshape(shape4)
    lap = jnp.einsum('ka,xkyb->xayb', slopes, weight4 * grad_x, precision=hp) + jnp.einsum('kb,xayk->xayb', slopes, weight4 * grad_y, precision=hp)
    return mass_w * values + scale * lap.reshape(row_count, col_count)

def diag_terms(flux_w, slopes):
    row_count, col_count = flux_w.shape
    shape4 = (row_count // 4, 4, col_count // 4, 4)
    weight4 = flux_w.reshape(shape4)
    hp = lax.Precision.HIGHEST
    squared = slopes * slopes
    terms = jnp.einsum('ka,xkyb->xayb', squared, weight4, precision=hp) + jnp.einsum('kb,xayk->xayb', squared, weight4, precision=hp)
    return terms.reshape(row_count, col_count)

def reference(forcing, metric, jacobian, mode_scale):
    slopes = jnp.asarray(gll_tables()[0], jnp.float32)
    row_w, row_mult = line_tables(metric.shape[0])
    col_w, col_mult = line_tables(metric.shape[1])
    grid_w = row_w[:, None] * col_w[None, :]
    inv_count = 1.0 / (row_mult[:, None] * col_mult[None, :])
    mass_w = jacobian * grid_w
    flux_w = metric * grid_w
    mass_diag = assemble(mass_w)
    lap_diag = assemble(diag_terms(flux_w, slopes))

    def solve_mode(member):
        source, scale = member
        rhs = assemble(source * mass_w)
        precond = mass_diag + scale * lap_diag
        solution = jnp.zeros_like(rhs)
        residual = rhs
        zvec = residual / precond
        direction = zvec
        rho_now = jnp.sum(residual * zvec * inv_count)
        for iteration in range(ITERS):
            image = assemble(apply_local(direction, scale, slopes, mass_w, flux_w))
            step_len = rho_now / jnp.sum(direction * image * inv_count)
            solution = solution + step_len * direction
            residual = residual - step_len * image
            zvec = residual / precond
            rho_next = jnp.sum(residual * zvec * inv_count)
            direction = zvec + rho_next / rho_now * direction
            rho_now = rho_next
        return (solution, residual)
    solution, residual = lax.map(solve_mode, (forcing, mode_scale))
    return (solution, residual)
```

```python
import functools
import math

import jax
import jax.numpy as jnp
import numpy as np
from jax import lax
from jax.experimental import pallas as pl
from jax.experimental.pallas import tpu as pltpu
from jax.sharding import PartitionSpec as P

ITERS = 3
GROUPS = 2
SIGMA = 1.25
LEVELS = 2 * ITERS
UNROLL = True
MESH = pl.DeviceIdType.MESH
LANES = 128
f32 = jnp.float32
bf16 = jnp.bfloat16


def gll_tables():
    points = np.array([-1.0, -1.0 / math.sqrt(5.0), 1.0 / math.sqrt(5.0), 1.0])
    weights = np.array([1.0 / 6.0, 5.0 / 6.0, 5.0 / 6.0, 1.0 / 6.0])
    factor = np.array(
        [np.prod([points[j] - points[m] for m in range(4) if m != j]) for j in range(4)]
    )
    slopes = np.zeros((4, 4))
    for i in range(4):
        for j in range(4):
            if i != j:
                slopes[i, j] = factor[i] / (factor[j] * (points[i] - points[j]))
        slopes[i, i] = sum((1.0 / (points[i] - points[m]) for m in range(4) if m != i))
    return (slopes, weights)


SLOPES, WEIGHTS = gll_tables()


def combo(coefs, parts):
    total = None
    for c, v in zip(coefs, parts):
        if abs(c) < 1e-12:
            continue
        term = v * f32(c)
        total = term if total is None else total + term
    return total


def kernel(
    nc, ns, modes, groups,
    scale_hbm, forcing_ref, metric_ref, jac_ref, grad_hbm, div_hbm,
    v0, v1, v2, last, diag, coef,
    w, invp, mass, flux, zcat, gout, sums,
    row_tx, row_rx, col_tx, col_rx, cor_rx, ar_tx, ar_rx,
    source, factors, grad_ref, div_ref, scale_ref,
    htx_sem, hrx_sem, atx_sem, arx_sem, in_sem, table_sem,
):
    rows, cols = metric_ref.shape
    q = rows // 4
    n = nc * ns
    half = cols - LANES
    tiles = cols // LANES
    per = modes // groups
    slots = row_tx.shape[2]
    loads, sources = [], []
    for c in range(tiles):
        cut = pl.ds(c * LANES, LANES)
        loads += [
            pltpu.make_async_copy(jac_ref.at[:, cut], factors.at[0, c], in_sem.at[0, c]),
            pltpu.make_async_copy(metric_ref.at[:, cut], factors.at[1, c], in_sem.at[1, c]),
        ]
        sources.append(
            pltpu.make_async_copy(forcing_ref.at[:, :, cut], source.at[c], in_sem.at[2, c]))
    div_load = pltpu.make_async_copy(div_hbm, div_ref, table_sem.at[0])
    grad_load = pltpu.make_async_copy(grad_hbm, grad_ref, table_sem.at[1])
    scale_load = pltpu.make_async_copy(scale_hbm, scale_ref, table_sem.at[2])
    for copy in loads + sources + [div_load, scale_load, grad_load]:
        copy.start()

    me_c, me_s = lax.axis_index("curve"), lax.axis_index("sub")
    me = me_c * ns + me_s
    up, down = lax.rem(me_c + nc - 1, nc), lax.rem(me_c + 1, nc)
    left, right = lax.rem(me_s + ns - 1, ns), lax.rem(me_s + 1, ns)

    def place(offset):
        target = lax.rem(me + offset, n)
        return (target // ns, lax.rem(target, ns))

    barrier = pltpu.get_barrier_semaphore()

    def greet(offset, carry):
        pl.semaphore_signal(barrier, inc=1, device_id=place(offset), device_id_type=MESH)
        return carry

    lax.fori_loop(1, n, greet, 0)

    lane_full = lax.broadcasted_iota(jnp.int32, (q, cols), 1)
    lane = lax.broadcasted_iota(jnp.int32, (q, LANES), 1)
    row_at = lax.broadcasted_iota(jnp.int32, (q, cols), 0)
    phase = lane_full % 4
    on_edge = (phase == 0) | (phase == 3)
    take_next = (phase == 3) & (lane_full != cols - 1)
    take_prev = (phase == 0) & (lane_full != 0)

    def load(ref, m):
        return [ref[m, p * q:(p + 1) * q, :] for p in range(4)]

    def save(ref, m, parts):
        for p in range(4):
            ref[m, p * q:(p + 1) * q, :] = parts[p]

    def load2(ref):
        return [ref[p * q:(p + 1) * q, :] for p in range(4)]

    def pack(k, m, slot, h, tops):
        lo, hi = tops
        row_tx[k, 0, pl.ds(slot, 1), :] = h[0][0:1, :]
        row_tx[k, 1, pl.ds(slot, 1), :] = h[3][q - 1:q, :]
        t0 = h[0] + jnp.where(row_at == 0, 0.0, pltpu.roll(h[3], 1, 0))
        t3 = h[3] + jnp.where(row_at == q - 1, 0.0, pltpu.roll(h[0], q - 1, 0))
        t = [t0, h[1], h[2], t3]
        save(w, m, t)
        for p in range(4):
            at = 4 * slot + p
            lo = jnp.where(lane == at, pltpu.roll(t[p][:, :LANES], at, 1), lo)
            hi = jnp.where(lane == at, pltpu.roll(t[p][:, half:], at + 1, 1), hi)
        return lo, hi

    def halo_copies(k):
        plan = [
            (row_tx.at[k, 0], row_rx.at[k, 1], (up, me_s)),
            (row_tx.at[k, 1], row_rx.at[k, 0], (down, me_s)),
            (col_tx.at[k, 0, pl.ds(0, 1)], cor_rx.at[k, 3], (up, left)),
            (col_tx.at[k, 1, pl.ds(0, 1)], cor_rx.at[k, 2], (up, right)),
            (col_tx.at[k, 0, pl.ds(q - 1, 1)], cor_rx.at[k, 1], (down, left)),
            (col_tx.at[k, 1, pl.ds(q - 1, 1)], cor_rx.at[k, 0], (down, right)),
            (col_tx.at[k, 0], col_rx.at[k, 1], (me_c, left)),
            (col_tx.at[k, 1], col_rx.at[k, 0], (me_c, right)),
        ]
        return [
            pltpu.make_async_remote_copy(
                src_ref=src, dst_ref=dst, send_sem=htx_sem.at[k, e], recv_sem=hrx_sem.at[k, e],
                device_id=where, device_id_type=MESH)
            for e, (src, dst, where) in enumerate(plan)
        ]

    def send(k, tops):
        col_tx[k, 0], col_tx[k, 1] = tops
        for copy in halo_copies(k):
            copy.start()

    def arrive(k):
        for copy in halo_copies(k):
            copy.wait_recv()
        ph = lax.broadcasted_iota(jnp.int32, (1, LANES), 1) % 4
        edge_row = lax.broadcasted_iota(jnp.int32, (q, LANES), 0)
        merged = []
        for side in range(2):
            above, below = cor_rx[k, side], cor_rx[k, 2 + side]
            above = jnp.where(ph == 0, pltpu.roll(above, LANES - 3, 1), 0.0)
            below = jnp.where(ph == 3, pltpu.roll(below, 3, 1), 0.0)
            c = col_rx[k, side]
            c = c + jnp.where(edge_row == 0, above, 0.0) + jnp.where(edge_row == q - 1, below, 0.0)
            merged.append(c)
        return merged

    def assembled(k, m, slot, merged):
        t = load(w, m)
        t[0] = t[0] + jnp.where(row_at == 0, row_rx[k, 0, pl.ds(slot, 1), :], 0.0)
        t[3] = t[3] + jnp.where(row_at == q - 1, row_rx[k, 1, pl.ds(slot, 1), :], 0.0)
        out = []
        for p in range(4):
            at = 4 * slot + p
            c = t[p] + jnp.where(
                take_next, pltpu.roll(t[p], cols - 1, 1),
                jnp.where(take_prev, pltpu.roll(t[p], 1, 1), 0.0))
            a = jnp.where(lane == 0, pltpu.roll(merged[0], LANES - at, 1), 0.0)
            b = jnp.where(lane == LANES - 1, pltpu.roll(merged[1], LANES - 1 - at, 1), 0.0)
            pieces = [c[:, e * LANES:(e + 1) * LANES] for e in range(tiles)]
            pieces[0] = pieces[0] + a
            pieces[-1] = pieces[-1] + b
            out.append(jnp.concatenate(pieces, axis=1))
        return out

    edge_w, mid_w = f32(1.0 / 6.0), f32(5.0 / 6.0)
    col_w = jnp.where(on_edge, edge_w, mid_w)
    mw, fw = [], []
    for copy in loads:
        copy.wait()
    for p in range(4):
        grid_w = col_w * (edge_w if p in (0, 3) else mid_w)
        mw.append(strided([factors.at[0, c] for c in range(tiles)], p, q) * grid_w)
        fw.append(strided([factors.at[1, c] for c in range(tiles)], p, q) * grid_w)
        mass[p * q:(p + 1) * q, :] = mw[p]
        flux[p * q:(p + 1) * q, :] = fw[p]
    zero = jnp.zeros((q, LANES), f32)
    tops = pack(0, modes, per, mw, (zero, zero))
    div_load.wait()
    table = div_ref[:cols, :].astype(f32) + div_ref[2 * cols:, :].astype(f32)
    by_cols = jnp.dot(flux[...], table * table, precision=lax.Precision.HIGHEST,
                      preferred_element_type=f32)
    squared = SLOPES * SLOPES
    lap = [combo(squared[:, a], fw) + by_cols[a * q:(a + 1) * q, :] for a in range(4)]
    tops = pack(0, modes + 1, per + 1, lap, tops)
    for copy in sources:
        copy.wait()
    for g in range(groups):

        def start_body(slot, carry, g=g):
            m = g * per + slot
            h = [strided([source.at[c, m] for c in range(tiles)], p, q)
                 * mass[p * q:(p + 1) * q, :] for p in range(4)]
            return pack(g, m, slot, h, carry)

        tops = lax.fori_loop(0, per, start_body, tops if g == 0 else (zero, zero), unroll=UNROLL)
        if g == 0:
            pl.semaphore_wait(barrier, n - 1)
        send(g, tops)
    scale_load.wait()
    grad_load.wait()

    basis = (v0, v1, v2)
    span = sums.shape[0] // LEVELS

    def fill(slot, parts):
        v = jnp.concatenate(parts, axis=0)
        top = v.astype(bf16)
        at = pl.ds(pl.multiple_of(slot * rows, rows), rows)
        zcat[at, :cols] = top
        zcat[at, cols:] = (v - top.astype(f32)).astype(bf16)

    def multiply(table_ref):
        gout[...] = (
            jnp.dot(zcat[...], table_ref[:2 * cols, :], preferred_element_type=f32)
            + jnp.dot(zcat[:, :cols], table_ref[2 * cols:, :], preferred_element_type=f32))

    for it in range(ITERS):
        for g in range(groups):
            base = g * per
            k = it * groups + g
            merged = arrive(k)
            if it == 0 and g == 0:
                for e in range(2):
                    save(diag, e, assembled(k, modes + e, per + e, merged))

            def first(slot, carry, it=it, k=k, base=base, merged=merged):
                m = base + slot
                ww = assembled(k, m, slot, merged)
                if it == 0:
                    inv = [1.0 / (u + scale_ref[m] * v)
                           for u, v in zip(load(diag, 0), load(diag, 1))]
                    save(invp, m, inv)
                    zz = [u * v for u, v in zip(ww, inv)]
                else:
                    zz = [u * v - f32(SIGMA) * o
                          for u, v, o in zip(ww, load(invp, m), load(basis[it - 1], m))]
                save(basis[it], m, zz)
                fill(slot, zz)
                rz = [u * v for u, v in zip(ww, zz)]
                rho = (rz[0] + rz[3]) * 0.5 + (rz[1] + rz[2])
                rho = jnp.where(on_edge, rho * 0.5, rho)
                sums[pl.ds(2 * it * span + m, 1), :] = jnp.sum(rho, axis=0, keepdims=True)
                f = load2(flux)
                fg = [f[a] * combo(SLOPES[a], zz) * scale_ref[m] for a in range(4)]
                ms = load2(mass)
                save(w, m, [ms[a] * zz[a] + combo(SLOPES[:, a], fg) for a in range(4)])
                return carry

            lax.fori_loop(0, per, first, 0, unroll=UNROLL)
            multiply(grad_ref)

            def second(slot, carry, base=base):
                grad = gout[pl.ds(pl.multiple_of(slot * rows, rows), rows), :]
                fill(slot, [flux[...] * grad * scale_ref[base + slot]])
                return carry

            lax.fori_loop(0, per, second, 0, unroll=UNROLL)
            multiply(div_ref)

            def third(slot, carry, it=it, k=k, base=base):
                m = base + slot
                zz = load(basis[it], m)
                h = [u + gout[pl.ds(pl.multiple_of(slot * rows + p * q, q), q), :]
                     for p, u in enumerate(load(w, m))]
                zh = zz[0] * h[0] + zz[1] * h[1] + zz[2] * h[2] + zz[3] * h[3]
                sums[pl.ds((2 * it + 1) * span + m, 1), :] = jnp.sum(zh, axis=0, keepdims=True)
                return pack(k + groups, m, slot, h, carry)

            tops = lax.fori_loop(0, per, third, (zero, zero), unroll=UNROLL)
            send(k + groups, tops)

    total_rows = sums.shape[0]
    wide = ar_tx.shape[1]
    eye = lax.broadcasted_iota(jnp.int32, (total_rows, wide), 0) == lax.broadcasted_iota(
        jnp.int32, (total_rows, wide), 1)
    part = jnp.sum(sums[...], axis=1, keepdims=True)
    line = jnp.sum(jnp.where(eye, part, 0.0), axis=0, keepdims=True)
    ar_tx[...] = line
    ar_rx[0:1, :] = line

    def spread(offset, carry):
        pltpu.make_async_remote_copy(
            src_ref=ar_tx, dst_ref=ar_rx.at[pl.ds(offset, 1)],
            send_sem=atx_sem, recv_sem=arx_sem,
            device_id=place(offset), device_id_type=MESH).start()
        return carry

    lax.fori_loop(1, n, spread, 0, unroll=True if n <= 32 else 1)

    for g in range(groups):
        k = ITERS * groups + g
        merged = arrive(k)

        def finish(slot, carry, g=g, k=k, merged=merged):
            m = g * per + slot
            save(last, m, assembled(k, m, slot, merged))
            return carry

        lax.fori_loop(0, per, finish, 0, unroll=UNROLL)

    gathered = ar_rx.at[pl.ds(1, n - 1)]
    pltpu.make_async_copy(gathered, gathered, arx_sem).wait()
    total = jnp.sum(ar_rx[...], axis=0, keepdims=True)
    solve(total, span, coef)

    for k in range((ITERS + 1) * groups):
        for copy in halo_copies(k):
            copy.wait_send()
    pltpu.make_async_copy(gathered, gathered, atx_sem).wait()


def solve(total, span, coef):
    wide = total.shape[1]
    live = lax.broadcasted_iota(jnp.int32, (1, wide), 1) < coef.shape[1]
    b0, a0, b1, a1, b2, a2 = [
        jnp.where(live, total if e == 0 else pltpu.roll(total, wide - e * span, 1), 1.0)
        for e in range(LEVELS)]
    sigma = f32(SIGMA)
    n1 = a0 - sigma * b0
    n2 = b1 - sigma * n1
    n3 = a1 - sigma * n2
    g02 = n3 + sigma * n2
    l1, l2 = b1 / a0, g02 / a0
    d1 = a1 - l1 * b1
    e12 = b2 - l1 * g02
    l3 = e12 / d1
    d2 = a2 - l2 * g02 - l3 * e12
    y1 = n1 - l1 * b0
    y2 = n2 - l2 * b0 - l3 * y1
    c2 = y2 / d2
    c1 = y1 / d1 - l3 * c2
    c0 = b0 / a0 - l1 * c1 - l2 * c2
    spot = (lax.broadcasted_iota(jnp.int32, (coef.shape[1], wide), 0)
            == lax.broadcasted_iota(jnp.int32, (coef.shape[1], wide), 1))
    for e, line in enumerate((c0, c1, c2, 1.0 - sigma * c0, c0 + sigma * c1)):
        tall = jnp.sum(jnp.where(spot, line, 0.0), axis=1, keepdims=True)
        coef[e] = jnp.broadcast_to(tall, coef.shape[1:])


def node_order(
    scale_hbm, v0, v1, v2, last, diag, coef, sol_ref, res_ref,
    sol_buf, res_buf, scale_ref, sem, scale_sem,
):
    modes, rows, cols = v0.shape
    q, tiles = rows // 4, cols // LANES
    scale_load = pltpu.make_async_copy(scale_hbm, scale_ref, scale_sem)
    scale_load.start()
    scale_load.wait()

    def stores(m):
        return [
            pltpu.make_async_copy(
                buf.at[c, m], out.at[m, :, pl.ds(c * LANES, LANES)], sem.at[k, c, m])
            for k, (buf, out) in enumerate(((sol_buf, sol_ref), (res_buf, res_ref)))
            for c in range(tiles)
        ]

    def body(m, carry):
        c0, c1, c2, k0, k1 = [coef[e, pl.ds(m, 1), :] for e in range(5)]
        for p in range(4):
            cut = slice(p * q, (p + 1) * q)
            a, b, c = v0[m, cut, :], v1[m, cut, :], v2[m, cut, :]
            x = c0 * a + c1 * b + c2 * c
            weight = diag[0, cut, :] + scale_ref[m] * diag[1, cut, :]
            r = weight * (k0 * a - k1 * b - c1 * c) - c2 * last[m, cut, :]
            for t in range(tiles):
                lanes = slice(t * LANES, (t + 1) * LANES)
                sol_buf[t, m, pl.ds(p, q, stride=4), :] = x[:, lanes]
                res_buf[t, m, pl.ds(p, q, stride=4), :] = r[:, lanes]
        for copy in stores(m):
            copy.start()
        return carry

    lax.fori_loop(0, modes, body, 0)

    def drain(m, carry):
        for copy in stores(m):
            copy.wait()
        return carry

    lax.fori_loop(0, modes, drain, 0)


def strided(refs, p, q):
    return jnp.concatenate([ref[pl.ds(p, q, stride=4), :] for ref in refs], axis=1)


def stack_table(table):
    top = table.astype(bf16)
    low = (table - top.astype(np.float32)).astype(bf16)
    return np.concatenate([top, top, low], axis=0)


def shards(nc, ns, forcing, metric, jacobian, mode_scale):
    modes, rows, cols = forcing.shape
    block = np.kron(np.eye(cols // 4), SLOPES).astype(np.float32)
    grad, div = stack_table(block.T), stack_table(block)
    n, q, tiles = nc * ns, rows // 4, cols // LANES
    groups = GROUPS if modes % GROUPS == 0 else 1
    per = modes // groups
    slots = -(-(per + 2) // 8) * 8
    vm = pl.BlockSpec(memory_space=pltpu.VMEM)
    hbm = pl.BlockSpec(memory_space=pltpu.HBM)
    rounds = (ITERS + 1) * groups
    span = -(-modes // 8) * 8
    wide = -(-LEVELS * span // LANES) * LANES
    field = pltpu.VMEM((modes, rows, cols), f32)
    split = pltpu.VMEM((tiles, modes, rows, LANES), f32)
    table = pltpu.VMEM(grad.shape, bf16)
    shape = jax.ShapeDtypeStruct(forcing.shape, f32)
    built = pl.pallas_call(
        functools.partial(kernel, nc, ns, modes, groups),
        out_shape=[shape] * 4 + [
            jax.ShapeDtypeStruct((2, rows, cols), f32),
            jax.ShapeDtypeStruct((5, span, cols), f32)],
        in_specs=[hbm] * 6,
        out_specs=[vm] * 6,
        scratch_shapes=[
            pltpu.VMEM((modes + 2, rows, cols), f32),
            field,
            pltpu.VMEM((rows, cols), f32),
            pltpu.VMEM((rows, cols), f32),
            pltpu.VMEM((per * rows, 2 * cols), bf16),
            pltpu.VMEM((per * rows, cols), f32),
            pltpu.VMEM((LEVELS * span, cols), f32),
            pltpu.VMEM((rounds, 2, slots, cols), f32),
            pltpu.VMEM((rounds, 2, slots, cols), f32),
            pltpu.VMEM((rounds, 2, q, LANES), f32),
            pltpu.VMEM((rounds, 2, q, LANES), f32),
            pltpu.VMEM((rounds, 4, 1, LANES), f32),
            pltpu.VMEM((1, wide), f32),
            pltpu.VMEM((n, wide), f32),
            split,
            pltpu.VMEM((2, tiles, rows, LANES), f32),
            table, table,
            pltpu.SMEM((modes,), f32),
            pltpu.SemaphoreType.DMA((rounds, 8)),
            pltpu.SemaphoreType.DMA((rounds, 8)),
            pltpu.SemaphoreType.DMA,
            pltpu.SemaphoreType.DMA,
            pltpu.SemaphoreType.DMA((3, tiles)),
            pltpu.SemaphoreType.DMA((3,)),
        ],
        compiler_params=pltpu.CompilerParams(
            collective_id=0, has_side_effects=True, vmem_limit_bytes=41943040),
    )(*[pltpu.with_memory_space_constraint(v, pltpu.HBM) for v in (mode_scale, forcing, metric, jacobian, jnp.asarray(grad), jnp.asarray(div))])
    return pl.pallas_call(
        node_order,
        out_shape=[shape] * 2,
        in_specs=[hbm] + [vm] * 6,
        out_specs=[hbm, hbm],
        scratch_shapes=[
            split, split, pltpu.SMEM((modes,), f32),
            pltpu.SemaphoreType.DMA((2, tiles, modes)), pltpu.SemaphoreType.DMA],
        compiler_params=pltpu.CompilerParams(vmem_limit_bytes=16 * 1024 * 1024),
    )(pltpu.with_memory_space_constraint(mode_scale, pltpu.HBM), *built)


def solution(mesh):
    placed = (P(None, "curve", "sub"), P("curve", "sub"), P("curve", "sub"), P())
    return jax.shard_map(
        functools.partial(shards, mesh.shape["curve"], mesh.shape["sub"]),
        mesh=mesh,
        in_specs=placed,
        out_specs=(P(None, "curve", "sub"), P(None, "curve", "sub")),
        check_vma=False,
    )
```

```python
import functools
import math

import jax
import jax.numpy as jnp
import numpy as np
from jax import lax
from jax.experimental import pallas as pl
from jax.experimental.pallas import tpu as pltpu
from jax.sharding import PartitionSpec as P

ITERS = 3
GROUPS = 2
SIGMA = 1.25
SUMS = 2 * ITERS
UNROLL = True
OUT_UNROLL = 4
MESH = pl.DeviceIdType.MESH
LANES = 128
f32 = jnp.float32
bf16 = jnp.bfloat16


def gll_tables():
    points = np.array([-1.0, -1.0 / math.sqrt(5.0), 1.0 / math.sqrt(5.0), 1.0])
    weights = np.array([1.0 / 6.0, 5.0 / 6.0, 5.0 / 6.0, 1.0 / 6.0])
    factor = np.array(
        [np.prod([points[j] - points[m] for m in range(4) if m != j]) for j in range(4)]
    )
    slopes = np.zeros((4, 4))
    for i in range(4):
        for j in range(4):
            if i != j:
                slopes[i, j] = factor[i] / (factor[j] * (points[i] - points[j]))
        slopes[i, i] = sum((1.0 / (points[i] - points[m]) for m in range(4) if m != i))
    return (slopes, weights)


SLOPES, WEIGHTS = gll_tables()


def combo(coefs, parts):
    total = None
    for c, v in zip(coefs, parts):
        if abs(c) < 1e-12:
            continue
        term = v * f32(c)
        total = term if total is None else total + term
    return total


def apply_line(table, v):
    phase = lax.broadcasted_iota(jnp.int32, (1, LANES), 1) % 4
    total = None
    for d in range(-3, 4):
        coef = jnp.zeros((1, LANES), f32)
        for p in range(4):
            if 0 <= p + d < 4 and abs(table[p, p + d]) > 1e-12:
                coef = jnp.where(phase == p, f32(table[p, p + d]), coef)
        moved = v if d == 0 else pltpu.roll(v, (LANES - d) % LANES, 1)
        total = coef * moved if total is None else total + coef * moved
    return total


def stiff_line(flux, v):
    return apply_line(SLOPES.T, flux * apply_line(SLOPES, v))


def kernel(
    nc, ns, modes, groups,
    scale_hbm, forcing_ref, metric_ref, jac_ref, grad_hbm, div_hbm,
    v0, v1, v2, last, diag, coef, edge_row, edge_col,
    w, invp, mass, flux, zcat, gout, sums,
    row_e, col_e, row_d, col_d, row_m, row_i, col_m, col_i, row_fix, col_fix, row_k, col_k,
    row_c, col_c,
    row_tx, row_rx, col_tx, col_rx, cor_rx, ar_tx, ar_rx,
    source, factors, grad_ref, div_ref, scale_ref,
    htx_sem, hrx_sem, atx_sem, arx_sem, in_sem, table_sem,
):
    rows, cols = metric_ref.shape
    q = rows // 4
    n = nc * ns
    half = cols - LANES
    tiles = cols // LANES
    per = modes // groups
    slots = row_tx.shape[2]
    loads, sources = [], []
    for c in range(tiles):
        cut = pl.ds(c * LANES, LANES)
        loads += [
            pltpu.make_async_copy(jac_ref.at[:, cut], factors.at[0, c], in_sem.at[0, c]),
            pltpu.make_async_copy(metric_ref.at[:, cut], factors.at[1, c], in_sem.at[1, c]),
        ]
        sources.append(
            pltpu.make_async_copy(forcing_ref.at[:, :, cut], source.at[c], in_sem.at[2, c]))
    div_load = pltpu.make_async_copy(div_hbm, div_ref, table_sem.at[0])
    grad_load = pltpu.make_async_copy(grad_hbm, grad_ref, table_sem.at[1])
    scale_load = pltpu.make_async_copy(scale_hbm, scale_ref, table_sem.at[2])
    for copy in loads + sources + [scale_load]:
        copy.start()

    me_c, me_s = lax.axis_index("curve"), lax.axis_index("sub")
    me = me_c * ns + me_s
    up, down = lax.rem(me_c + nc - 1, nc), lax.rem(me_c + 1, nc)
    left, right = lax.rem(me_s + ns - 1, ns), lax.rem(me_s + 1, ns)

    def place(offset):
        target = lax.rem(me + offset, n)
        return (target // ns, lax.rem(target, ns))

    barrier = pltpu.get_barrier_semaphore()

    def greet(offset, carry):
        pl.semaphore_signal(barrier, inc=1, device_id=place(offset), device_id_type=MESH)
        return carry

    lax.fori_loop(1, n, greet, 0)

    def iota(shape, axis):
        return lax.broadcasted_iota(jnp.int32, shape, axis)

    def ways(shape):
        at = iota(shape, 1)
        return (at % 4 == 3) & (at != cols - 1), (at % 4 == 0) & (at != 0)

    lane_full = iota((q, cols), 1)
    lane = iota((q, LANES), 1)
    row_at = iota((q, cols), 0)
    edge_at = iota((q, LANES), 0)
    phase = lane_full % 4
    on_edge = (phase == 0) | (phase == 3)
    inside = (lane_full != 0) & (lane_full != cols - 1)

    def load(ref, m):
        return [ref[m, p * q:(p + 1) * q, :] for p in range(4)]

    def save(ref, m, parts):
        for p in range(4):
            ref[m, p * q:(p + 1) * q, :] = parts[p]

    def load2(ref):
        return [ref[p * q:(p + 1) * q, :] for p in range(4)]

    def join_cols(t, shape):
        take_next, take_prev = ways(shape)
        return t + jnp.where(
            take_next, pltpu.roll(t, cols - 1, 1),
            jnp.where(take_prev, pltpu.roll(t, 1, 1), 0.0))

    def join_rows(c):
        ph = lane % 4
        after = pltpu.roll(pltpu.roll(c, LANES - (LANES - 3), 1), q - 1, 0)
        before = pltpu.roll(pltpu.roll(c, LANES - 3, 1), 1, 0)
        return c + jnp.where((ph == 3) & (edge_at != q - 1), after,
                             jnp.where((ph == 0) & (edge_at != 0), before, 0.0))

    def pack(rows_ref, m, slot, h, tops):
        lo, hi = tops
        rows_ref[0, pl.ds(slot, 1), :] = h[0][0:1, :]
        rows_ref[1, pl.ds(slot, 1), :] = h[3][q - 1:q, :]
        save(w, m, joined(h))
        for p in range(4):
            at = 4 * slot + p
            lo = jnp.where(lane == at, pltpu.roll(h[p][:, :LANES], at, 1), lo)
            hi = jnp.where(lane == at, pltpu.roll(h[p][:, half:], at + 1, 1), hi)
        return lo, hi

    def halo_copies(k):
        plan = [
            (row_tx.at[k, 0], row_rx.at[k, 1], (up, me_s)),
            (row_tx.at[k, 1], row_rx.at[k, 0], (down, me_s)),
            (col_tx.at[k, 0, pl.ds(0, 1)], cor_rx.at[k, 3], (up, left)),
            (col_tx.at[k, 1, pl.ds(0, 1)], cor_rx.at[k, 2], (up, right)),
            (col_tx.at[k, 0, pl.ds(q - 1, 1)], cor_rx.at[k, 1], (down, left)),
            (col_tx.at[k, 1, pl.ds(q - 1, 1)], cor_rx.at[k, 0], (down, right)),
            (col_tx.at[k, 0], col_rx.at[k, 1], (me_c, left)),
            (col_tx.at[k, 1], col_rx.at[k, 0], (me_c, right)),
        ]
        return [
            pltpu.make_async_remote_copy(
                src_ref=src, dst_ref=dst, send_sem=htx_sem.at[k, e], recv_sem=hrx_sem.at[k, e],
                device_id=where, device_id_type=MESH)
            for e, (src, dst, where) in enumerate(plan)
        ]

    def send(k):
        for copy in halo_copies(k):
            copy.start()

    ends = ((0, 0), (q - 1, 3))
    tall = iota((slots, LANES), 0)
    wide_lane = iota((slots, LANES), 1)

    def to_rows(line, p0, target):
        found = jnp.where(wide_lane == 4 * tall + p0, line, 0.0)
        found = jnp.sum(found, axis=1, keepdims=True)
        return jnp.where(wide_lane == target, found, 0.0)

    def to_cols(block, p0, target):
        at = wide_lane == 4 * tall + p0
        spread = jnp.broadcast_to(block[:, target:target + 1], (slots, LANES))
        return jnp.sum(jnp.where(at, spread, 0.0), axis=0, keepdims=True)

    def at_sides(lo, hi):
        middle = [jnp.zeros((slots, LANES), f32)] * (tiles - 2)
        return jnp.concatenate([lo] + middle + [hi], axis=1)

    def side_tile(block, side):
        return block[:, half:] if side else block[:, :LANES]

    def arrive(k):
        for copy in halo_copies(k):
            copy.wait_recv()
        ph = iota((1, LANES), 1) % 4
        merged = []
        for side in range(2):
            above, below = cor_rx[k, side], cor_rx[k, 2 + side]
            above = jnp.where(ph == 0, pltpu.roll(above, LANES - 3, 1), 0.0)
            below = jnp.where(ph == 3, pltpu.roll(below, 3, 1), 0.0)
            c = col_rx[k, side]
            merged.append(
                c + jnp.where(edge_at == 0, above, 0.0) + jnp.where(edge_at == q - 1, below, 0.0))
        on_rows, on_cols = [], []
        for end, (at, p0) in enumerate(ends):
            t = join_cols(row_tx[k, end] + row_rx[k, end], (slots, cols))
            on_rows.append(t + at_sides(
                to_rows(merged[0][at:at + 1, :], p0, 0),
                to_rows(merged[1][at:at + 1, :], p0, LANES - 1)))
        for side in range(2):
            c = col_tx[k, side] + merged[side]
            for end, (at, p0) in enumerate(ends):
                line = to_cols(side_tile(row_rx[k, end], side), p0, (LANES - 1) * side)
                c = c + jnp.where(edge_at == at, line, 0.0)
            on_cols.append(c)
        return on_rows, on_cols

    def fixed(m):
        t = load(w, m)
        for p in range(4):
            pieces = [t[p][:, e * LANES:(e + 1) * LANES] for e in range(tiles)]
            for side, e in ((0, 0), (1, tiles - 1)):
                value = pltpu.roll(col_fix[side], LANES - 4 * m - p, 1)[:, 0:1]
                pieces[e] = pieces[e] + value * col_k[side, p]
            t[p] = jnp.concatenate(pieces, axis=1)
            blocks = [t[p][:8, :], t[p][8:q - 8, :], t[p][q - 8:, :]]
            for end, (at, p0) in enumerate(ends):
                line = row_fix[end, p, pl.ds(m, 1), :]
                spot = 7 * end if p != p0 else 1 + 5 * end
                blocks[2 * end] = blocks[2 * end] + jnp.where(row_at[:8, :] == spot, line, 0.0)
            t[p] = jnp.concatenate(blocks, axis=0)
        return t

    def joined(h):
        t0 = h[0] + jnp.where(row_at == 0, 0.0, pltpu.roll(h[3], 1, 0))
        t3 = h[3] + jnp.where(row_at == q - 1, 0.0, pltpu.roll(h[0], q - 1, 0))
        return [join_cols(t, (q, cols)) for t in (t0, h[1], h[2], t3)]

    def clear(parts):
        keep = [inside] * 4
        keep[0] = inside & (row_at != 0)
        keep[3] = inside & (row_at != q - 1)
        return [jnp.where(k, u, 0.0) for k, u in zip(keep, parts)]

    edge_w, mid_w = f32(1.0 / 6.0), f32(5.0 / 6.0)
    grid_lane = jnp.where(on_edge, edge_w, mid_w)
    mw, fw = [], []
    for copy in loads:
        copy.wait()
    for p in range(4):
        grid_w = grid_lane * (edge_w if p in (0, 3) else mid_w)
        mw.append(strided([factors.at[0, c] for c in range(tiles)], p, q) * grid_w)
        fw.append(strided([factors.at[1, c] for c in range(tiles)], p, q) * grid_w)
        mass[p * q:(p + 1) * q, :] = mw[p]
        flux[p * q:(p + 1) * q, :] = fw[p]
    zero = jnp.zeros((q, LANES), f32)
    tops = pack(row_tx.at[0], modes, modes, mw, (zero, zero))
    squared = SLOPES * SLOPES

    def per_line(fn, block):
        return jnp.concatenate(
            [fn(block[:, e * LANES:(e + 1) * LANES], e) for e in range(tiles)], axis=1)

    lap = [combo(squared[:, a], fw) + per_line(lambda v, e: apply_line(squared.T, v), fw[a])
           for a in range(4)]
    tops = pack(row_tx.at[0], modes + 1, modes + 1, lap, tops)
    for copy in sources:
        copy.wait()
    grad_load.start()
    div_load.start()

    def start_body(m, carry):
        h = [strided([source.at[c, m] for c in range(tiles)], p, q)
             * mass[p * q:(p + 1) * q, :] for p in range(4)]
        return pack(row_tx.at[0], m, m, h, carry)

    tops = lax.fori_loop(0, modes, start_body, tops, unroll=2)
    for side in range(2):
        col_tx[0, side] = join_rows(tops[side])
    pl.semaphore_wait(barrier, n - 1)
    send(0)
    scale_load.wait()

    basis = (v0, v1, v2)
    span = sums.shape[0] // SUMS
    scale_rows = jnp.zeros((slots, LANES), f32)
    scale_lanes = jnp.zeros((1, LANES), f32)
    lane_one = iota((1, LANES), 1)
    for m in range(modes):
        scale_rows = jnp.where(tall == m, scale_ref[m], scale_rows)
        scale_lanes = jnp.where(lane_one // 4 == m, scale_ref[m], scale_lanes)
    scale_rows = jnp.concatenate([scale_rows] * tiles, axis=1)

    ffull, mfull = load2(flux), load2(mass)
    line_lane = iota((1, cols), 1)
    not_corner = (line_lane != 0) & (line_lane != cols - 1)
    for end, (at, p0) in enumerate(ends):
        cut = [f[at:at + 1, :] for f in ffull]
        row_c[end, 0:1, :] = cut[p0]
        row_c[end, 1:2, :] = mfull[p0][at:at + 1, :]
        row_c[end, 2:3, :] = jnp.where(not_corner, combo(SLOPES[:, p0] ** 2, cut), 0.0)
        for p in range(4):
            far = p if p != p0 else 3 - p0
            row_k[end, p:p + 1, :] = join_cols(
                combo(SLOPES[:, p0] * SLOPES[:, far], cut), (1, cols))
    for side in range(2):
        fc, mc, dc = zero, zero, zero
        reach = []
        for p in range(4):
            f = side_tile(ffull[p], side)
            base = half and (LANES - 4) * side
            cells = [jnp.broadcast_to(f[:, base + b:base + b + 1], (q, LANES)) for b in range(4)]
            b0 = 3 * side
            mass_cell = side_tile(mfull[p], side)[:, base + b0:base + b0 + 1]
            mine = lane % 4 == p
            fc = jnp.where(mine, cells[b0], fc)
            mc = jnp.where(mine, mass_cell, mc)
            dc = jnp.where(mine, combo(SLOPES[:, b0] ** 2, cells), dc)
            block = zero
            for b in range(4):
                if b != b0:
                    hit = lane == base + b
                    if b == 3 - b0:
                        hit = hit | (lane == base + b + 1 - 2 * side)
                    block = jnp.where(hit, combo(SLOPES[:, b0] * SLOPES[:, b], cells), block)
            reach.append(block)
        col_k[side, 0] = reach[0] + jnp.where(edge_at == 0, 0.0, pltpu.roll(reach[3], 1, 0))
        col_k[side, 1], col_k[side, 2] = reach[1], reach[2]
        col_k[side, 3] = reach[3] + jnp.where(
            edge_at == q - 1, 0.0, pltpu.roll(reach[0], q - 1, 0))
        for at, p0 in ends:
            dc = jnp.where((edge_at == at) & (lane % 4 == p0), 0.0, dc)
        col_c[side, 0], col_c[side, 1], col_c[side, 2] = fc, mc, dc

    def fill(b, slot, parts):
        v = jnp.concatenate(parts, axis=0)
        top = v.astype(bf16)
        at = pl.ds(pl.multiple_of(slot * rows, rows), rows)
        zcat[b, at, :cols] = top
        zcat[b, at, cols:] = (v - top.astype(f32)).astype(bf16)

    def multiply(b, table_ref):
        gout[b] = (
            jnp.dot(zcat[b], table_ref[:2 * cols, :], preferred_element_type=f32)
            + jnp.dot(zcat[b, :, :cols], table_ref[2 * cols:, :], preferred_element_type=f32))

    def build(it):
        tops = (zero, zero)
        for b in range(groups):
            base = b * per

            def first(slot, carry, b=b, base=base):
                m = base + slot
                t = load(w, m) if it == 0 else fixed(m)
                if it == 0:
                    inv = clear([1.0 / (u + scale_ref[m] * v)
                                 for u, v in zip(load(diag, 0), load(diag, 1))])
                    save(invp, m, inv)
                    zz = [u * v for u, v in zip(t, inv)]
                else:
                    zz = [u * v - f32(SIGMA) * o
                          for u, v, o in zip(t, load(invp, m), load(basis[it - 1], m))]
                save(basis[it], m, zz)
                fill(b, slot, zz)
                rz = [u * v for u, v in zip(t, zz)]
                rho = (rz[0] + rz[3]) * 0.5 + (rz[1] + rz[2])
                rho = jnp.where(on_edge, rho * 0.5, rho)
                sums[pl.ds(2 * it * span + m, 1), :] = jnp.sum(rho, axis=0, keepdims=True)
                f = load2(flux)
                fg = [f[a] * combo(SLOPES[a], zz) * scale_ref[m] for a in range(4)]
                ms = load2(mass)
                save(w, m, [ms[a] * zz[a] + combo(SLOPES[:, a], fg) for a in range(4)])
                return carry

            lax.fori_loop(0, per, first, 0, unroll=True)
            if it == 0 and b == 0:
                grad_load.wait()
                div_load.wait()
            multiply(b, grad_ref)

            def second(slot, carry, b=b, base=base):
                grad = gout[b, pl.ds(pl.multiple_of(slot * rows, rows), rows), :]
                fill(b, slot, [flux[...] * grad * scale_ref[base + slot]])
                return carry

            lax.fori_loop(0, per, second, 0, unroll=True)
            multiply(b, div_ref)

            def third(slot, carry, b=b, base=base):
                m = base + slot
                zz = load(basis[it], m)
                h = [u + gout[b, pl.ds(pl.multiple_of(slot * rows + p * q, q), q), :]
                     for p, u in enumerate(load(w, m))]
                zh = zz[0] * h[0] + zz[1] * h[1] + zz[2] * h[2] + zz[3] * h[3]
                sums[pl.ds((2 * it + 1) * span + m, 1), :] = jnp.sum(zh, axis=0, keepdims=True)
                return pack(row_e, m, m, h, carry)

            tops = lax.fori_loop(0, per, third, tops, unroll=True)
        col_e[0], col_e[1] = tops

    row_weight = jnp.where((line_lane % 4 == 0) | (line_lane % 4 == 3), 0.25, 0.5).astype(f32)
    corner = ((edge_at == 0) & (lane % 4 == 0)) | ((edge_at == q - 1) & (lane % 4 == 3))
    col_weight = jnp.where((lane % 4 == 0) | (lane % 4 == 3), 0.25, 0.5).astype(f32)
    col_weight = jnp.where(corner, 0.0, col_weight)
    own_slot = wide_lane // 4 == tall

    def fold(e, on_rows, on_cols):
        at = slice(e * span, e * span + slots)
        sums[at, :] = sums[at, :] + (on_rows[0] + on_rows[1])
        line = jnp.sum(on_cols[0] + on_cols[1], axis=0, keepdims=True)
        sums[at, :LANES] = sums[at, :LANES] + jnp.where(own_slot, line, 0.0)

    def step(it):
        on_rows, on_cols = arrive(it)
        row_now, col_now, row_s, col_s = [], [], [], []
        for i in range(2):
            if it == 0:
                t = on_rows[i]
                weight = t[modes:modes + 1, :] + scale_rows * t[modes + 1:modes + 2, :]
                row_m[i], row_i[i] = weight, 1.0 / weight
                c = on_cols[i]
                md, ld = zero, zero
                for p in range(4):
                    a, b = 4 * modes + p, 4 * modes + 4 + p
                    md = jnp.where(lane % 4 == p, c[:, a:a + 1], md)
                    ld = jnp.where(lane % 4 == p, c[:, b:b + 1], ld)
                weight = md + scale_lanes * ld
                col_m[i], col_i[i] = weight, 1.0 / weight
            r, c = on_rows[i] * row_i[i], on_cols[i] * col_i[i]
            if it > 0:
                r, c = r - f32(SIGMA) * row_d[it - 1, i], c - f32(SIGMA) * col_d[it - 1, i]
            row_d[it, i], col_d[it, i] = r, c
            row_now.append(r)
            col_now.append(c)
            row_s.append(per_line(
                lambda v, e, i=i: stiff_line(row_c[i, 0:1, e * LANES:(e + 1) * LANES], v), r))
            col_s.append(stiff_line(col_c[i, 0], c))
        row_out, col_out = [], []
        for end, (at, p0) in enumerate(ends):
            across = at_sides(
                to_rows(col_s[0][at:at + 1, :], p0, 0),
                to_rows(col_s[1][at:at + 1, :], p0, LANES - 1))
            r = row_now[end]
            row_out.append(
                row_e[end] + row_c[end, 1:2, :] * r
                + scale_rows * (row_c[end, 2:3, :] * r + row_s[end] + across))
        for side in range(2):
            total = col_s[side] + col_c[side, 2] * col_now[side]
            for end, (at, p0) in enumerate(ends):
                line = to_cols(side_tile(row_s[end], side), p0, (LANES - 1) * side)
                total = total + jnp.where((edge_at == at) & (lane % 4 == p0), line, 0.0)
            col_out.append(
                col_e[side] + col_c[side, 1] * col_now[side] + scale_lanes * total)
        for i in range(2):
            row_tx[it + 1, i] = row_out[i]
            col_tx[it + 1, i] = join_rows(col_out[i])
        if it < ITERS - 1:
            send(it + 1)
        fold(2 * it,
             [row_weight * u * v for u, v in zip(row_now, on_rows)],
             [col_weight * u * v for u, v in zip(col_now, on_cols)])
        fold(2 * it + 1,
             [u * (a + b) for u, a, b in zip(row_now, [row_e[0], row_e[1]], row_out)],
             [jnp.where(corner, 0.0, u * (a + b))
              for u, a, b in zip(col_now, [col_e[0], col_e[1]], col_out)])
        lines.append(reduce_sums(it))
        if it == ITERS - 1:
            spread_sums()
            send(it + 1)
        for i, (at, p0) in enumerate(ends):
            col_fix[i] = scale_lanes * col_now[i]
            for p in range(4):
                row_fix[i, p] = scale_rows * row_now[i] * row_k[i, p:p + 1, :]

    wide = ar_tx.shape[1]
    gathered = ar_rx.at[pl.ds(1, n - 1)]
    lines = []

    def reduce_sums(it):
        base = 2 * it * span
        eye = iota((2 * span, wide), 0) + base == iota((2 * span, wide), 1)
        part = jnp.sum(sums[base:base + 2 * span, :], axis=1, keepdims=True)
        return jnp.sum(jnp.where(eye, part, 0.0), axis=0, keepdims=True)

    def spread_sums():
        line = sum(lines)
        ar_tx[...] = line
        ar_rx[0:1, :] = line

        def spread(offset, carry):
            pltpu.make_async_remote_copy(
                src_ref=ar_tx, dst_ref=ar_rx.at[pl.ds(offset, 1)],
                send_sem=atx_sem, recv_sem=arx_sem,
                device_id=place(offset), device_id_type=MESH).start()
            return carry

        lax.fori_loop(1, n, spread, 0, unroll=True if n <= 32 else 1)

    sums[...] = jnp.zeros_like(sums)
    for e in range(2):
        save(diag, e, load(w, modes + e))
    for it in range(ITERS):
        build(it)
        step(it)

    def finish(m, carry):
        save(last, m, clear(fixed(m)))
        return carry

    lax.fori_loop(0, modes, finish, 0, unroll=2)
    on_rows, on_cols = arrive(ITERS)
    pltpu.make_async_copy(gathered, gathered, arx_sem).wait()
    total = jnp.sum(ar_rx[...], axis=0, keepdims=True)
    solve(total, span, coef)
    on_lanes = [
        jnp.sum(jnp.where(own_slot, coef[e, :slots, :LANES], 0.0), axis=0, keepdims=True)
        for e in range(5)]
    for i in range(2):
        for ref, given, prior, weight, (c0, c1, c2, k0, k1) in (
                (edge_row, on_rows[i], row_d, row_m[i], [coef[e, :slots, :] for e in range(5)]),
                (edge_col, on_cols[i], col_d, col_m[i], on_lanes)):
            a, b, c = prior[0, i], prior[1, i], prior[2, i]
            ref[0, i] = c0 * a + c1 * b + c2 * c
            ref[1, i] = weight * (k0 * a - k1 * b - c1 * c) - c2 * given

    for k in range(ITERS + 1):
        for copy in halo_copies(k):
            copy.wait_send()
    pltpu.make_async_copy(gathered, gathered, atx_sem).wait()


def solve(total, span, coef):
    wide = total.shape[1]
    live = lax.broadcasted_iota(jnp.int32, (1, wide), 1) < coef.shape[1]
    b0, a0, b1, a1, b2, a2 = [
        jnp.where(live, total if e == 0 else pltpu.roll(total, wide - e * span, 1), 1.0)
        for e in range(SUMS)]
    sigma = f32(SIGMA)
    n1 = a0 - sigma * b0
    n2 = b1 - sigma * n1
    n3 = a1 - sigma * n2
    g02 = n3 + sigma * n2
    l1, l2 = b1 / a0, g02 / a0
    d1 = a1 - l1 * b1
    e12 = b2 - l1 * g02
    l3 = e12 / d1
    d2 = a2 - l2 * g02 - l3 * e12
    y1 = n1 - l1 * b0
    y2 = n2 - l2 * b0 - l3 * y1
    c2 = y2 / d2
    c1 = y1 / d1 - l3 * c2
    c0 = b0 / a0 - l1 * c1 - l2 * c2
    spot = (lax.broadcasted_iota(jnp.int32, (coef.shape[1], wide), 0)
            == lax.broadcasted_iota(jnp.int32, (coef.shape[1], wide), 1))
    for e, line in enumerate((c0, c1, c2, 1.0 - sigma * c0, c0 + sigma * c1)):
        tall = jnp.sum(jnp.where(spot, line, 0.0), axis=1, keepdims=True)
        coef[e] = jnp.broadcast_to(tall, coef.shape[1:])


def node_order(
    scale_hbm, v0, v1, v2, last, diag, coef, edge_row, edge_col, sol_ref, res_ref,
    sol_buf, res_buf, scale_ref, sem, scale_sem,
):
    modes, rows, cols = v0.shape
    q, tiles = rows // 4, cols // LANES
    scale_load = pltpu.make_async_copy(scale_hbm, scale_ref, scale_sem)
    scale_load.start()
    scale_load.wait()

    lane = lax.broadcasted_iota(jnp.int32, (q, LANES), 1)

    def stores(m):
        return [
            pltpu.make_async_copy(
                buf.at[c, m], out.at[m, :, pl.ds(c * LANES, LANES)], sem.at[k, c, m])
            for k, (buf, out) in enumerate(((sol_buf, sol_ref), (res_buf, res_ref)))
            for c in range(tiles)
        ]

    def body(m, carry):
        c0, c1, c2, k0, k1 = [coef[e, pl.ds(m, 1), :] for e in range(5)]
        for p in range(4):
            cut = slice(p * q, (p + 1) * q)
            a, b, c = v0[m, cut, :], v1[m, cut, :], v2[m, cut, :]
            x = c0 * a + c1 * b + c2 * c
            weight = diag[0, cut, :] + scale_ref[m] * diag[1, cut, :]
            r = weight * (k0 * a - k1 * b - c1 * c) - c2 * last[m, cut, :]
            for field, (buf, whole) in enumerate(((sol_buf, x), (res_buf, r))):
                for t in range(tiles):
                    piece = whole[:, t * LANES:(t + 1) * LANES]
                    for side, own in ((0, 0), (1, tiles - 1)):
                        if t == own:
                            spot = (LANES - 1) * side
                            line = pltpu.roll(
                                edge_col[field, side], spot + LANES - 4 * m - p, 1)
                            piece = piece + jnp.where(lane == spot, line, 0.0)
                    buf[t, m, pl.ds(p, q, stride=4), :] = piece
        for field, buf in enumerate((sol_buf, res_buf)):
            for end, at in ((0, 0), (1, rows - 1)):
                line = edge_row[field, end, pl.ds(m, 1), :]
                for t in range(tiles):
                    buf[t, m, at:at + 1, :] = line[:, t * LANES:(t + 1) * LANES]
        for copy in stores(m):
            copy.start()
        return carry

    lax.fori_loop(0, modes, body, 0, unroll=OUT_UNROLL)

    def drain(m, carry):
        for copy in stores(m):
            copy.wait()
        return carry

    lax.fori_loop(0, modes, drain, 0)


def strided(refs, p, q):
    return jnp.concatenate([ref[pl.ds(p, q, stride=4), :] for ref in refs], axis=1)


def stack_table(table):
    top = table.astype(bf16)
    low = (table - top.astype(np.float32)).astype(bf16)
    return np.concatenate([top, top, low], axis=0)


def shards(nc, ns, forcing, metric, jacobian, mode_scale):
    modes, rows, cols = forcing.shape
    block = np.kron(np.eye(cols // 4), SLOPES).astype(np.float32)
    grad, div = stack_table(block.T), stack_table(block)
    n, q, tiles = nc * ns, rows // 4, cols // LANES
    groups = GROUPS if modes % GROUPS == 0 else 1
    per = modes // groups
    slots = -(-(modes + 2) // 8) * 8
    vm = pl.BlockSpec(memory_space=pltpu.VMEM)
    hbm = pl.BlockSpec(memory_space=pltpu.HBM)
    rounds = ITERS + 1
    span = slots
    wide = -(-SUMS * span // LANES) * LANES
    field = pltpu.VMEM((modes, rows, cols), f32)
    split = pltpu.VMEM((tiles, modes, rows, LANES), f32)
    table = pltpu.VMEM(grad.shape, bf16)
    shape = jax.ShapeDtypeStruct(forcing.shape, f32)

    def on_rows(*lead):
        return pltpu.VMEM((*lead, slots, cols), f32)

    def on_cols(*lead):
        return pltpu.VMEM((*lead, q, LANES), f32)

    built = pl.pallas_call(
        functools.partial(kernel, nc, ns, modes, groups),
        out_shape=[shape] * 4 + [
            jax.ShapeDtypeStruct((2, rows, cols), f32),
            jax.ShapeDtypeStruct((5, span, cols), f32),
            jax.ShapeDtypeStruct((2, 2, slots, cols), f32),
            jax.ShapeDtypeStruct((2, 2, q, LANES), f32)],
        in_specs=[hbm] * 6,
        out_specs=[vm] * 8,
        scratch_shapes=[
            pltpu.VMEM((modes + 2, rows, cols), f32),
            field,
            pltpu.VMEM((rows, cols), f32),
            pltpu.VMEM((rows, cols), f32),
            pltpu.VMEM((groups, per * rows, 2 * cols), bf16),
            pltpu.VMEM((groups, per * rows, cols), f32),
            pltpu.VMEM((SUMS * span, cols), f32),
            on_rows(2), on_cols(2),
            on_rows(ITERS, 2), on_cols(ITERS, 2),
            on_rows(2), on_rows(2), on_cols(2), on_cols(2),
            on_rows(2, 4), on_cols(2),
            pltpu.VMEM((2, 8, cols), f32),
            on_cols(2, 4),
            pltpu.VMEM((2, 8, cols), f32),
            on_cols(2, 3),
            on_rows(rounds, 2), on_rows(rounds, 2),
            on_cols(rounds, 2), on_cols(rounds, 2),
            pltpu.VMEM((rounds, 4, 1, LANES), f32),
            pltpu.VMEM((1, wide), f32),
            pltpu.VMEM((n, wide), f32),
            split,
            pltpu.VMEM((2, tiles, rows, LANES), f32),
            table, table,
            pltpu.SMEM((modes,), f32),
            pltpu.SemaphoreType.DMA((rounds, 8)),
            pltpu.SemaphoreType.DMA((rounds, 8)),
            pltpu.SemaphoreType.DMA,
            pltpu.SemaphoreType.DMA,
            pltpu.SemaphoreType.DMA((3, tiles)),
            pltpu.SemaphoreType.DMA((3,)),
        ],
        compiler_params=pltpu.CompilerParams(
            collective_id=0, has_side_effects=True, vmem_limit_bytes=41943040),
    )(*[pltpu.with_memory_space_constraint(v, pltpu.HBM) for v in (mode_scale, forcing, metric, jacobian, jnp.asarray(grad), jnp.asarray(div))])
    return pl.pallas_call(
        node_order,
        out_shape=[shape] * 2,
        in_specs=[hbm] + [vm] * 8,
        out_specs=[hbm, hbm],
        scratch_shapes=[
            split, split, pltpu.SMEM((modes,), f32),
            pltpu.SemaphoreType.DMA((2, tiles, modes)), pltpu.SemaphoreType.DMA],
        compiler_params=pltpu.CompilerParams(vmem_limit_bytes=16 * 1024 * 1024),
    )(pltpu.with_memory_space_constraint(mode_scale, pltpu.HBM), *built)


def solution(mesh):
    placed = (P(None, "curve", "sub"), P("curve", "sub"), P("curve", "sub"), P())
    return jax.shard_map(
        functools.partial(shards, mesh.shape["curve"], mesh.shape["sub"]),
        mesh=mesh,
        in_specs=placed,
        out_specs=(P(None, "curve", "sub"), P(None, "curve", "sub")),
        check_vma=False,
    )
```

```python
import functools
import math

import jax
import jax.numpy as jnp
import numpy as np
from jax import lax
from jax.experimental import pallas as pl
from jax.experimental.pallas import tpu as pltpu
from jax.sharding import PartitionSpec as P

ITERS = 3
GROUPS = 2
SIGMA = 1.25
SUMS = 2 * ITERS
UNROLL = True
OUT_UNROLL = 4
MESH = pl.DeviceIdType.MESH
LANES = 128
f32 = jnp.float32
bf16 = jnp.bfloat16


def gll_tables():
    points = np.array([-1.0, -1.0 / math.sqrt(5.0), 1.0 / math.sqrt(5.0), 1.0])
    weights = np.array([1.0 / 6.0, 5.0 / 6.0, 5.0 / 6.0, 1.0 / 6.0])
    factor = np.array(
        [np.prod([points[j] - points[m] for m in range(4) if m != j]) for j in range(4)]
    )
    slopes = np.zeros((4, 4))
    for i in range(4):
        for j in range(4):
            if i != j:
                slopes[i, j] = factor[i] / (factor[j] * (points[i] - points[j]))
        slopes[i, i] = sum((1.0 / (points[i] - points[m]) for m in range(4) if m != i))
    return (slopes, weights)


SLOPES, WEIGHTS = gll_tables()


def combo(coefs, parts):
    total = None
    for c, v in zip(coefs, parts):
        if abs(c) < 1e-12:
            continue
        term = v * f32(c)
        total = term if total is None else total + term
    return total


def apply_line(table, v):
    phase = lax.broadcasted_iota(jnp.int32, (1, LANES), 1) % 4
    total = None
    for d in range(-3, 4):
        coef = jnp.zeros((1, LANES), f32)
        for p in range(4):
            if 0 <= p + d < 4 and abs(table[p, p + d]) > 1e-12:
                coef = jnp.where(phase == p, f32(table[p, p + d]), coef)
        moved = v if d == 0 else pltpu.roll(v, (LANES - d) % LANES, 1)
        total = coef * moved if total is None else total + coef * moved
    return total


def bands(flux):
    out = []
    for d in range(-3, 4):
        table = np.zeros((4, 4))
        for p in range(4):
            if 0 <= p + d < 4:
                table[p] = SLOPES[:, p] * SLOPES[:, p + d]
        out.append(apply_line(table, flux))
    return out


def stiff_line(band, v):
    total = band(3) * v
    for d in (-3, -2, -1, 1, 2, 3):
        total = total + band(3 + d) * pltpu.roll(v, (LANES - d) % LANES, 1)
    return total


def kernel(
    nc, ns, modes, groups,
    scale_hbm, forcing_ref, metric_ref, jac_ref, grad_hbm, div_hbm,
    v0, v1, v2, last, diag, coef, edge_row, edge_col,
    w, invp, mass, flux, zcat, gout, sums,
    row_e, col_e, row_d, col_d, row_m, row_i, col_m, col_i, row_fix, col_fix, row_k, col_k,
    row_c, col_c,
    row_tx, row_rx, col_tx, col_rx, cor_rx, ar_tx, ar_rx,
    source, factors, grad_ref, div_ref, scale_ref,
    htx_sem, hrx_sem, atx_sem, arx_sem, in_sem, table_sem,
):
    rows, cols = metric_ref.shape
    q = rows // 4
    n = nc * ns
    half = cols - LANES
    tiles = cols // LANES
    per = modes // groups
    slots = row_tx.shape[2]
    loads, sources = [], []
    for c in range(tiles):
        cut = pl.ds(c * LANES, LANES)
        loads += [
            pltpu.make_async_copy(jac_ref.at[:, cut], factors.at[0, c], in_sem.at[0, c]),
            pltpu.make_async_copy(metric_ref.at[:, cut], factors.at[1, c], in_sem.at[1, c]),
        ]
        sources.append(
            pltpu.make_async_copy(forcing_ref.at[:, :, cut], source.at[c], in_sem.at[2, c]))
    div_load = pltpu.make_async_copy(div_hbm, div_ref, table_sem.at[0])
    grad_load = pltpu.make_async_copy(grad_hbm, grad_ref, table_sem.at[1])
    scale_load = pltpu.make_async_copy(scale_hbm, scale_ref, table_sem.at[2])
    for copy in loads + sources + [scale_load]:
        copy.start()

    me_c, me_s = lax.axis_index("curve"), lax.axis_index("sub")
    me = me_c * ns + me_s
    up, down = lax.rem(me_c + nc - 1, nc), lax.rem(me_c + 1, nc)
    left, right = lax.rem(me_s + ns - 1, ns), lax.rem(me_s + 1, ns)

    def place(offset):
        target = lax.rem(me + offset, n)
        return (target // ns, lax.rem(target, ns))

    barrier = pltpu.get_barrier_semaphore()

    def greet(offset, carry):
        pl.semaphore_signal(barrier, inc=1, device_id=place(offset), device_id_type=MESH)
        return carry

    lax.fori_loop(1, n, greet, 0, unroll=True if n <= 32 else 1)

    def iota(shape, axis):
        return lax.broadcasted_iota(jnp.int32, shape, axis)

    def ways(shape):
        at = iota(shape, 1)
        return (at % 4 == 3) & (at != cols - 1), (at % 4 == 0) & (at != 0)

    lane_full = iota((q, cols), 1)
    lane = iota((q, LANES), 1)
    row_at = iota((q, cols), 0)
    edge_at = iota((q, LANES), 0)
    phase = lane_full % 4
    on_edge = (phase == 0) | (phase == 3)
    inside = (lane_full != 0) & (lane_full != cols - 1)

    def load(ref, m):
        return [ref[m, p * q:(p + 1) * q, :] for p in range(4)]

    def save(ref, m, parts):
        for p in range(4):
            ref[m, p * q:(p + 1) * q, :] = parts[p]

    def load2(ref):
        return [ref[p * q:(p + 1) * q, :] for p in range(4)]

    def join_cols(t, shape):
        take_next, take_prev = ways(shape)
        return t + jnp.where(
            take_next, pltpu.roll(t, cols - 1, 1),
            jnp.where(take_prev, pltpu.roll(t, 1, 1), 0.0))

    def join_rows(c):
        ph = lane % 4
        after = pltpu.roll(pltpu.roll(c, LANES - (LANES - 3), 1), q - 1, 0)
        before = pltpu.roll(pltpu.roll(c, LANES - 3, 1), 1, 0)
        return c + jnp.where((ph == 3) & (edge_at != q - 1), after,
                             jnp.where((ph == 0) & (edge_at != 0), before, 0.0))

    def pack(rows_ref, m, slot, h, tops):
        lo, hi = tops
        rows_ref[0, pl.ds(slot, 1), :] = h[0][0:1, :]
        rows_ref[1, pl.ds(slot, 1), :] = h[3][q - 1:q, :]
        save(w, m, joined(h))
        for p in range(4):
            at = 4 * slot + p
            lo = jnp.where(lane == at, pltpu.roll(h[p][:, :LANES], at, 1), lo)
            hi = jnp.where(lane == at, pltpu.roll(h[p][:, half:], at + 1, 1), hi)
        return lo, hi

    def halo_copies(k):
        plan = [
            (row_tx.at[k, 0], row_rx.at[k, 1], (up, me_s)),
            (row_tx.at[k, 1], row_rx.at[k, 0], (down, me_s)),
            (col_tx.at[k, 0, pl.ds(0, 1)], cor_rx.at[k, 3], (up, left)),
            (col_tx.at[k, 1, pl.ds(0, 1)], cor_rx.at[k, 2], (up, right)),
            (col_tx.at[k, 0, pl.ds(q - 1, 1)], cor_rx.at[k, 1], (down, left)),
            (col_tx.at[k, 1, pl.ds(q - 1, 1)], cor_rx.at[k, 0], (down, right)),
            (col_tx.at[k, 0], col_rx.at[k, 1], (me_c, left)),
            (col_tx.at[k, 1], col_rx.at[k, 0], (me_c, right)),
        ]
        return [
            pltpu.make_async_remote_copy(
                src_ref=src, dst_ref=dst, send_sem=htx_sem.at[k, e], recv_sem=hrx_sem.at[k, e],
                device_id=where, device_id_type=MESH)
            for e, (src, dst, where) in enumerate(plan)
        ]

    def send(k):
        for copy in halo_copies(k):
            copy.start()

    ends = ((0, 0), (q - 1, 3))
    tall = iota((slots, LANES), 0)
    wide_lane = iota((slots, LANES), 1)

    def to_rows(line, p0, target):
        found = jnp.where(wide_lane == 4 * tall + p0, line, 0.0)
        found = jnp.sum(found, axis=1, keepdims=True)
        return jnp.where(wide_lane == target, found, 0.0)

    def to_cols(block, p0, target):
        at = wide_lane == 4 * tall + p0
        spread = jnp.broadcast_to(block[:, target:target + 1], (slots, LANES))
        return jnp.sum(jnp.where(at, spread, 0.0), axis=0, keepdims=True)

    def at_sides(lo, hi):
        middle = [jnp.zeros((slots, LANES), f32)] * (tiles - 2)
        return jnp.concatenate([lo] + middle + [hi], axis=1)

    def side_tile(block, side):
        return block[:, half:] if side else block[:, :LANES]

    def arrive(k):
        for copy in halo_copies(k):
            copy.wait_recv()
        ph = iota((1, LANES), 1) % 4
        merged = []
        for side in range(2):
            above, below = cor_rx[k, side], cor_rx[k, 2 + side]
            above = jnp.where(ph == 0, pltpu.roll(above, LANES - 3, 1), 0.0)
            below = jnp.where(ph == 3, pltpu.roll(below, 3, 1), 0.0)
            c = col_rx[k, side]
            merged.append(
                c + jnp.where(edge_at == 0, above, 0.0) + jnp.where(edge_at == q - 1, below, 0.0))
        on_rows, on_cols = [], []
        for end, (at, p0) in enumerate(ends):
            t = join_cols(row_tx[k, end] + row_rx[k, end], (slots, cols))
            on_rows.append(t + at_sides(
                to_rows(merged[0][at:at + 1, :], p0, 0),
                to_rows(merged[1][at:at + 1, :], p0, LANES - 1)))
        for side in range(2):
            c = col_tx[k, side] + merged[side]
            for end, (at, p0) in enumerate(ends):
                line = to_cols(side_tile(row_rx[k, end], side), p0, (LANES - 1) * side)
                c = c + jnp.where(edge_at == at, line, 0.0)
            on_cols.append(c)
        return on_rows, on_cols

    def fixed(m):
        t = load(w, m)
        for p in range(4):
            pieces = [t[p][:, e * LANES:(e + 1) * LANES] for e in range(tiles)]
            for side, e in ((0, 0), (1, tiles - 1)):
                value = pltpu.roll(col_fix[side], LANES - 4 * m - p, 1)[:, 0:1]
                pieces[e] = pieces[e] + value * col_k[side, p]
            t[p] = jnp.concatenate(pieces, axis=1)
            blocks = [t[p][:8, :], t[p][8:q - 8, :], t[p][q - 8:, :]]
            for end, (at, p0) in enumerate(ends):
                line = row_fix[end, p, pl.ds(m, 1), :]
                spot = 7 * end if p != p0 else 1 + 5 * end
                blocks[2 * end] = blocks[2 * end] + jnp.where(row_at[:8, :] == spot, line, 0.0)
            t[p] = jnp.concatenate(blocks, axis=0)
        return t

    def joined(h):
        t0 = h[0] + jnp.where(row_at == 0, 0.0, pltpu.roll(h[3], 1, 0))
        t3 = h[3] + jnp.where(row_at == q - 1, 0.0, pltpu.roll(h[0], q - 1, 0))
        return [join_cols(t, (q, cols)) for t in (t0, h[1], h[2], t3)]

    def clear(parts):
        keep = [inside] * 4
        keep[0] = inside & (row_at != 0)
        keep[3] = inside & (row_at != q - 1)
        return [jnp.where(k, u, 0.0) for k, u in zip(keep, parts)]

    edge_w, mid_w = f32(1.0 / 6.0), f32(5.0 / 6.0)
    grid_lane = jnp.where(on_edge, edge_w, mid_w)
    mw, fw = [], []
    for copy in loads:
        copy.wait()
    for p in range(4):
        grid_w = grid_lane * (edge_w if p in (0, 3) else mid_w)
        mw.append(strided([factors.at[0, c] for c in range(tiles)], p, q) * grid_w)
        fw.append(strided([factors.at[1, c] for c in range(tiles)], p, q) * grid_w)
        mass[p * q:(p + 1) * q, :] = mw[p]
        flux[p * q:(p + 1) * q, :] = fw[p]
    zero = jnp.zeros((q, LANES), f32)
    tops = pack(row_tx.at[0], modes, modes, mw, (zero, zero))
    squared = SLOPES * SLOPES

    def per_line(fn, block):
        return jnp.concatenate(
            [fn(block[:, e * LANES:(e + 1) * LANES], e) for e in range(tiles)], axis=1)

    lap = [combo(squared[:, a], fw) + per_line(lambda v, e: apply_line(squared.T, v), fw[a])
           for a in range(4)]
    tops = pack(row_tx.at[0], modes + 1, modes + 1, lap, tops)
    for copy in sources:
        copy.wait()
    grad_load.start()
    div_load.start()

    def start_body(m, carry):
        h = [strided([source.at[c, m] for c in range(tiles)], p, q)
             * mass[p * q:(p + 1) * q, :] for p in range(4)]
        return pack(row_tx.at[0], m, m, h, carry)

    tops = lax.fori_loop(0, modes, start_body, tops, unroll=2)
    for side in range(2):
        col_tx[0, side] = join_rows(tops[side])
    pl.semaphore_wait(barrier, n - 1)
    send(0)
    scale_load.wait()

    basis = (v0, v1, v2)
    span = sums.shape[0] // SUMS
    scale_rows = jnp.zeros((slots, LANES), f32)
    scale_lanes = jnp.zeros((1, LANES), f32)
    lane_one = iota((1, LANES), 1)
    for m in range(modes):
        scale_rows = jnp.where(tall == m, scale_ref[m], scale_rows)
        scale_lanes = jnp.where(lane_one // 4 == m, scale_ref[m], scale_lanes)
    scale_rows = jnp.concatenate([scale_rows] * tiles, axis=1)
    coef[5] = scale_rows

    ffull, mfull = load2(flux), load2(mass)
    line_lane = iota((1, cols), 1)
    not_corner = (line_lane != 0) & (line_lane != cols - 1)
    for end, (at, p0) in enumerate(ends):
        cut = [f[at:at + 1, :] for f in ffull]
        pieces = [bands(cut[p0][:, e * LANES:(e + 1) * LANES]) for e in range(tiles)]
        for d in range(7):
            row_c[end, d:d + 1, :] = jnp.concatenate([b[d] for b in pieces], axis=1)
        row_c[end, 3:4, :] = row_c[end, 3:4, :] + jnp.where(
            not_corner, combo(SLOPES[:, p0] ** 2, cut), 0.0)
        row_c[end, 7:8, :] = mfull[p0][at:at + 1, :]
        for p in range(4):
            far = p if p != p0 else 3 - p0
            row_k[end, p:p + 1, :] = join_cols(
                combo(SLOPES[:, p0] * SLOPES[:, far], cut), (1, cols))
    for side in range(2):
        fc, mc, dc = zero, zero, zero
        reach = []
        for p in range(4):
            f = side_tile(ffull[p], side)
            base = half and (LANES - 4) * side
            cells = [jnp.broadcast_to(f[:, base + b:base + b + 1], (q, LANES)) for b in range(4)]
            b0 = 3 * side
            mass_cell = side_tile(mfull[p], side)[:, base + b0:base + b0 + 1]
            mine = lane % 4 == p
            fc = jnp.where(mine, cells[b0], fc)
            mc = jnp.where(mine, mass_cell, mc)
            dc = jnp.where(mine, combo(SLOPES[:, b0] ** 2, cells), dc)
            block = zero
            for b in range(4):
                if b != b0:
                    hit = lane == base + b
                    if b == 3 - b0:
                        hit = hit | (lane == base + b + 1 - 2 * side)
                    block = jnp.where(hit, combo(SLOPES[:, b0] * SLOPES[:, b], cells), block)
            reach.append(block)
        col_k[side, 0] = reach[0] + jnp.where(edge_at == 0, 0.0, pltpu.roll(reach[3], 1, 0))
        col_k[side, 1], col_k[side, 2] = reach[1], reach[2]
        col_k[side, 3] = reach[3] + jnp.where(
            edge_at == q - 1, 0.0, pltpu.roll(reach[0], q - 1, 0))
        for at, p0 in ends:
            dc = jnp.where((edge_at == at) & (lane % 4 == p0), 0.0, dc)
        for d, band in enumerate(bands(fc)):
            col_c[side, d] = band + dc if d == 3 else band
        col_c[side, 7] = mc

    def fill(b, slot, parts):
        v = jnp.concatenate(parts, axis=0)
        top = v.astype(bf16)
        at = pl.ds(pl.multiple_of(slot * rows, rows), rows)
        zcat[b, at, :cols] = top
        zcat[b, at, cols:] = (v - top.astype(f32)).astype(bf16)

    def multiply(b, table_ref):
        gout[b] = (
            jnp.dot(zcat[b], table_ref[:2 * cols, :], preferred_element_type=f32)
            + jnp.dot(zcat[b, :, :cols], table_ref[2 * cols:, :], preferred_element_type=f32))

    def build(it):
        tops = (zero, zero)
        for b in range(groups):
            base = b * per

            def first(slot, carry, b=b, base=base):
                m = base + slot
                t = load(w, m) if it == 0 else fixed(m)
                if it == 0:
                    inv = clear([1.0 / (u + scale_ref[m] * v)
                                 for u, v in zip(load(diag, 0), load(diag, 1))])
                    save(invp, m, inv)
                    zz = [u * v for u, v in zip(t, inv)]
                else:
                    zz = [u * v - f32(SIGMA) * o
                          for u, v, o in zip(t, load(invp, m), load(basis[it - 1], m))]
                save(basis[it], m, zz)
                fill(b, slot, zz)
                rz = [u * v for u, v in zip(t, zz)]
                rho = (rz[0] + rz[3]) * 0.5 + (rz[1] + rz[2])
                rho = jnp.where(on_edge, rho * 0.5, rho)
                sums[pl.ds(2 * it * span + m, 1), :] = jnp.sum(rho, axis=0, keepdims=True)
                f = load2(flux)
                fg = [f[a] * combo(SLOPES[a], zz) * scale_ref[m] for a in range(4)]
                ms = load2(mass)
                save(w, m, [ms[a] * zz[a] + combo(SLOPES[:, a], fg) for a in range(4)])
                return carry

            lax.fori_loop(0, per, first, 0, unroll=True)
            if it == 0 and b == 0:
                grad_load.wait()
                div_load.wait()
            multiply(b, grad_ref)

            def second(slot, carry, b=b, base=base):
                grad = gout[b, pl.ds(pl.multiple_of(slot * rows, rows), rows), :]
                fill(b, slot, [flux[...] * grad * scale_ref[base + slot]])
                return carry

            lax.fori_loop(0, per, second, 0, unroll=True)
            multiply(b, div_ref)

            def third(slot, carry, b=b, base=base):
                m = base + slot
                zz = load(basis[it], m)
                h = [u + gout[b, pl.ds(pl.multiple_of(slot * rows + p * q, q), q), :]
                     for p, u in enumerate(load(w, m))]
                zh = zz[0] * h[0] + zz[1] * h[1] + zz[2] * h[2] + zz[3] * h[3]
                sums[pl.ds((2 * it + 1) * span + m, 1), :] = jnp.sum(zh, axis=0, keepdims=True)
                return pack(row_e, m, m, h, carry)

            tops = lax.fori_loop(0, per, third, tops, unroll=True)
        col_e[0], col_e[1] = tops

    row_weight = jnp.where((line_lane % 4 == 0) | (line_lane % 4 == 3), 0.25, 0.5).astype(f32)
    corner = ((edge_at == 0) & (lane % 4 == 0)) | ((edge_at == q - 1) & (lane % 4 == 3))
    col_weight = jnp.where((lane % 4 == 0) | (lane % 4 == 3), 0.25, 0.5).astype(f32)
    col_weight = jnp.where(corner, 0.0, col_weight)
    own_slot = wide_lane // 4 == tall

    def fold(e, on_rows, on_cols):
        at = slice(e * span, e * span + slots)
        sums[at, :] = sums[at, :] + (on_rows[0] + on_rows[1])
        line = jnp.sum(on_cols[0] + on_cols[1], axis=0, keepdims=True)
        sums[at, :LANES] = sums[at, :LANES] + jnp.where(own_slot, line, 0.0)

    def step(it):
        on_rows, on_cols = arrive(it)
        row_now, col_now, row_s, col_s = [], [], [], []
        for i in range(2):
            if it == 0:
                t = on_rows[i]
                weight = t[modes:modes + 1, :] + scale_rows * t[modes + 1:modes + 2, :]
                row_m[i], row_i[i] = weight, 1.0 / weight
                c = on_cols[i]
                md, ld = zero, zero
                for p in range(4):
                    a, b = 4 * modes + p, 4 * modes + 4 + p
                    md = jnp.where(lane % 4 == p, c[:, a:a + 1], md)
                    ld = jnp.where(lane % 4 == p, c[:, b:b + 1], ld)
                weight = md + scale_lanes * ld
                col_m[i], col_i[i] = weight, 1.0 / weight
            r, c = on_rows[i] * row_i[i], on_cols[i] * col_i[i]
            if it > 0:
                r, c = r - f32(SIGMA) * row_d[it - 1, i], c - f32(SIGMA) * col_d[it - 1, i]
            row_d[it, i], col_d[it, i] = r, c
            row_now.append(r)
            col_now.append(c)
            row_s.append(per_line(
                lambda v, e, i=i: stiff_line(
                    lambda d: row_c[i, d:d + 1, e * LANES:(e + 1) * LANES], v), r))
            col_s.append(stiff_line(lambda d, i=i: col_c[i, d], c))
        row_out, col_out = [], []
        for end, (at, p0) in enumerate(ends):
            across = at_sides(
                to_rows(col_s[0][at:at + 1, :], p0, 0),
                to_rows(col_s[1][at:at + 1, :], p0, LANES - 1))
            r = row_now[end]
            row_out.append(
                row_e[end] + row_c[end, 7:8, :] * r + scale_rows * (row_s[end] + across))
        for side in range(2):
            total = col_s[side]
            for end, (at, p0) in enumerate(ends):
                line = to_cols(side_tile(row_s[end], side), p0, (LANES - 1) * side)
                total = total + jnp.where((edge_at == at) & (lane % 4 == p0), line, 0.0)
            col_out.append(
                col_e[side] + col_c[side, 7] * col_now[side] + scale_lanes * total)
        for i in range(2):
            row_tx[it + 1, i] = row_out[i]
            col_tx[it + 1, i] = join_rows(col_out[i])
        if it < ITERS - 1:
            send(it + 1)
        fold(2 * it,
             [row_weight * u * v for u, v in zip(row_now, on_rows)],
             [col_weight * u * v for u, v in zip(col_now, on_cols)])
        fold(2 * it + 1,
             [u * (a + b) for u, a, b in zip(row_now, [row_e[0], row_e[1]], row_out)],
             [jnp.where(corner, 0.0, u * (a + b))
              for u, a, b in zip(col_now, [col_e[0], col_e[1]], col_out)])
        lines.append(reduce_sums(it))
        if it == ITERS - 1:
            spread_sums()
            send(it + 1)
        for i, (at, p0) in enumerate(ends):
            col_fix[i] = scale_lanes * col_now[i]
            for p in range(4):
                row_fix[i, p] = scale_rows * row_now[i] * row_k[i, p:p + 1, :]

    wide = ar_tx.shape[1]
    gathered = ar_rx.at[pl.ds(1, n - 1)]
    lines = []

    def reduce_sums(it):
        base = 2 * it * span
        eye = iota((2 * span, wide), 0) + base == iota((2 * span, wide), 1)
        part = jnp.sum(sums[base:base + 2 * span, :], axis=1, keepdims=True)
        return jnp.sum(jnp.where(eye, part, 0.0), axis=0, keepdims=True)

    def spread_sums():
        line = sum(lines)
        ar_tx[...] = line
        ar_rx[0:1, :] = line

        def spread(i, carry):
            offset = jnp.where(i % 2 == 1, (i + 1) // 2, n - i // 2)
            pltpu.make_async_remote_copy(
                src_ref=ar_tx, dst_ref=ar_rx.at[pl.ds(offset, 1)],
                send_sem=atx_sem, recv_sem=arx_sem,
                device_id=place(offset), device_id_type=MESH).start()
            return carry

        lax.fori_loop(1, n, spread, 0, unroll=True if n <= 32 else 1)

    sums[...] = jnp.zeros_like(sums)
    for e in range(2):
        save(diag, e, load(w, modes + e))
    for it in range(ITERS):
        build(it)
        step(it)

    def finish(m, carry):
        save(last, m, clear(fixed(m)))
        return carry

    lax.fori_loop(0, modes, finish, 0, unroll=2)
    on_rows, on_cols = arrive(ITERS)
    pltpu.make_async_copy(gathered, gathered, arx_sem).wait()
    total = jnp.sum(ar_rx[...], axis=0, keepdims=True)
    solve(total, span, coef)
    on_lanes = [
        jnp.sum(jnp.where(own_slot, coef[e, :slots, :LANES], 0.0), axis=0, keepdims=True)
        for e in range(5)]
    for i in range(2):
        for ref, given, prior, weight, (c0, c1, c2, k0, k1) in (
                (edge_row, on_rows[i], row_d, row_m[i], [coef[e, :slots, :] for e in range(5)]),
                (edge_col, on_cols[i], col_d, col_m[i], on_lanes)):
            a, b, c = prior[0, i], prior[1, i], prior[2, i]
            ref[0, i] = c0 * a + c1 * b + c2 * c
            ref[1, i] = weight * (k0 * a - k1 * b - c1 * c) - c2 * given

    for k in range(ITERS + 1):
        for copy in halo_copies(k):
            copy.wait_send()
    pltpu.make_async_copy(gathered, gathered, atx_sem).wait()


def solve(total, span, coef):
    wide = total.shape[1]
    live = lax.broadcasted_iota(jnp.int32, (1, wide), 1) < coef.shape[1]
    b0, a0, b1, a1, b2, a2 = [
        jnp.where(live, total if e == 0 else pltpu.roll(total, wide - e * span, 1), 1.0)
        for e in range(SUMS)]
    sigma = f32(SIGMA)
    n1 = a0 - sigma * b0
    n2 = b1 - sigma * n1
    n3 = a1 - sigma * n2
    g02 = n3 + sigma * n2
    l1, l2 = b1 / a0, g02 / a0
    d1 = a1 - l1 * b1
    e12 = b2 - l1 * g02
    l3 = e12 / d1
    d2 = a2 - l2 * g02 - l3 * e12
    y1 = n1 - l1 * b0
    y2 = n2 - l2 * b0 - l3 * y1
    c2 = y2 / d2
    c1 = y1 / d1 - l3 * c2
    c0 = b0 / a0 - l1 * c1 - l2 * c2
    spot = (lax.broadcasted_iota(jnp.int32, (coef.shape[1], wide), 0)
            == lax.broadcasted_iota(jnp.int32, (coef.shape[1], wide), 1))
    for e, line in enumerate((c0, c1, c2, 1.0 - sigma * c0, c0 + sigma * c1)):
        tall = jnp.sum(jnp.where(spot, line, 0.0), axis=1, keepdims=True)
        coef[e] = jnp.broadcast_to(tall, coef.shape[1:])


def node_order(
    v0, v1, v2, last, diag, coef, edge_row, edge_col, sol_ref, res_ref,
    sol_buf, res_buf, sem,
):
    modes, rows, cols = v0.shape
    q, tiles = rows // 4, cols // LANES

    lane = lax.broadcasted_iota(jnp.int32, (q, LANES), 1)

    def stores(m):
        return [
            pltpu.make_async_copy(
                buf.at[c, m], out.at[m, :, pl.ds(c * LANES, LANES)], sem.at[k, c, m])
            for k, (buf, out) in enumerate(((sol_buf, sol_ref), (res_buf, res_ref)))
            for c in range(tiles)
        ]

    def body(m, carry):
        c0, c1, c2, k0, k1, scale = [coef[e, pl.ds(m, 1), :] for e in range(6)]
        for p in range(4):
            cut = slice(p * q, (p + 1) * q)
            a, b, c = v0[m, cut, :], v1[m, cut, :], v2[m, cut, :]
            x = c0 * a + c1 * b + c2 * c
            weight = diag[0, cut, :] + scale * diag[1, cut, :]
            r = weight * (k0 * a - k1 * b - c1 * c) - c2 * last[m, cut, :]
            for field, (buf, whole) in enumerate(((sol_buf, x), (res_buf, r))):
                for t in range(tiles):
                    piece = whole[:, t * LANES:(t + 1) * LANES]
                    for side, own in ((0, 0), (1, tiles - 1)):
                        if t == own:
                            spot = (LANES - 1) * side
                            line = pltpu.roll(
                                edge_col[field, side], spot + LANES - 4 * m - p, 1)
                            piece = piece + jnp.where(lane == spot, line, 0.0)
                    buf[t, m, pl.ds(p, q, stride=4), :] = piece
        for field, buf in enumerate((sol_buf, res_buf)):
            for end, at in ((0, 0), (1, rows - 1)):
                line = edge_row[field, end, pl.ds(m, 1), :]
                for t in range(tiles):
                    buf[t, m, at:at + 1, :] = line[:, t * LANES:(t + 1) * LANES]
        for copy in stores(m):
            copy.start()
        return carry

    lax.fori_loop(0, modes, body, 0, unroll=OUT_UNROLL)

    def drain(m, carry):
        for copy in stores(m):
            copy.wait()
        return carry

    lax.fori_loop(0, modes, drain, 0)


def strided(refs, p, q):
    return jnp.concatenate([ref[pl.ds(p, q, stride=4), :] for ref in refs], axis=1)


def stack_table(table):
    top = table.astype(bf16)
    low = (table - top.astype(np.float32)).astype(bf16)
    return np.concatenate([top, top, low], axis=0)


def shards(nc, ns, forcing, metric, jacobian, mode_scale):
    modes, rows, cols = forcing.shape
    block = np.kron(np.eye(cols // 4), SLOPES).astype(np.float32)
    grad, div = stack_table(block.T), stack_table(block)
    n, q, tiles = nc * ns, rows // 4, cols // LANES
    groups = GROUPS if modes % GROUPS == 0 else 1
    per = modes // groups
    slots = -(-(modes + 2) // 8) * 8
    vm = pl.BlockSpec(memory_space=pltpu.VMEM)
    hbm = pl.BlockSpec(memory_space=pltpu.HBM)
    rounds = ITERS + 1
    span = slots
    wide = -(-SUMS * span // LANES) * LANES
    field = pltpu.VMEM((modes, rows, cols), f32)
    split = pltpu.VMEM((tiles, modes, rows, LANES), f32)
    table = pltpu.VMEM(grad.shape, bf16)
    shape = jax.ShapeDtypeStruct(forcing.shape, f32)

    def on_rows(*lead):
        return pltpu.VMEM((*lead, slots, cols), f32)

    def on_cols(*lead):
        return pltpu.VMEM((*lead, q, LANES), f32)

    built = pl.pallas_call(
        functools.partial(kernel, nc, ns, modes, groups),
        out_shape=[shape] * 4 + [
            jax.ShapeDtypeStruct((2, rows, cols), f32),
            jax.ShapeDtypeStruct((6, span, cols), f32),
            jax.ShapeDtypeStruct((2, 2, slots, cols), f32),
            jax.ShapeDtypeStruct((2, 2, q, LANES), f32)],
        in_specs=[hbm] * 6,
        out_specs=[vm] * 8,
        scratch_shapes=[
            pltpu.VMEM((modes + 2, rows, cols), f32),
            field,
            pltpu.VMEM((rows, cols), f32),
            pltpu.VMEM((rows, cols), f32),
            pltpu.VMEM((groups, per * rows, 2 * cols), bf16),
            pltpu.VMEM((groups, per * rows, cols), f32),
            pltpu.VMEM((SUMS * span, cols), f32),
            on_rows(2), on_cols(2),
            on_rows(ITERS, 2), on_cols(ITERS, 2),
            on_rows(2), on_rows(2), on_cols(2), on_cols(2),
            on_rows(2, 4), on_cols(2),
            pltpu.VMEM((2, 8, cols), f32),
            on_cols(2, 4),
            pltpu.VMEM((2, 8, cols), f32),
            on_cols(2, 8),
            on_rows(rounds, 2), on_rows(rounds, 2),
            on_cols(rounds, 2), on_cols(rounds, 2),
            pltpu.VMEM((rounds, 4, 1, LANES), f32),
            pltpu.VMEM((1, wide), f32),
            pltpu.VMEM((n, wide), f32),
            split,
            pltpu.VMEM((2, tiles, rows, LANES), f32),
            table, table,
            pltpu.SMEM((modes,), f32),
            pltpu.SemaphoreType.DMA((rounds, 8)),
            pltpu.SemaphoreType.DMA((rounds, 8)),
            pltpu.SemaphoreType.DMA,
            pltpu.SemaphoreType.DMA,
            pltpu.SemaphoreType.DMA((3, tiles)),
            pltpu.SemaphoreType.DMA((3,)),
        ],
        compiler_params=pltpu.CompilerParams(
            collective_id=0, has_side_effects=True, vmem_limit_bytes=41943040),
    )(*[pltpu.with_memory_space_constraint(v, pltpu.HBM) for v in (mode_scale, forcing, metric, jacobian, jnp.asarray(grad), jnp.asarray(div))])
    return pl.pallas_call(
        node_order,
        out_shape=[shape] * 2,
        in_specs=[vm] * 8,
        out_specs=[hbm, hbm],
        scratch_shapes=[
            split, split, pltpu.SemaphoreType.DMA((2, tiles, modes))],
        compiler_params=pltpu.CompilerParams(vmem_limit_bytes=16 * 1024 * 1024),
    )(*built)


def solution(mesh):
    placed = (P(None, "curve", "sub"), P("curve", "sub"), P("curve", "sub"), P())
    return jax.shard_map(
        functools.partial(shards, mesh.shape["curve"], mesh.shape["sub"]),
        mesh=mesh,
        in_specs=placed,
        out_specs=(P(None, "curve", "sub"), P(None, "curve", "sub")),
        check_vma=False,
    )
```

```python
import functools
import math

import jax
import jax.numpy as jnp
import numpy as np
from jax import lax
from jax.experimental import pallas as pl
from jax.experimental.pallas import tpu as pltpu
from jax.sharding import PartitionSpec as P

ITERS = 3
GROUPS = 2
SIGMA = 1.25
SUMS = 2 * ITERS
UNROLL = True
OUT_UNROLL = 4
MESH = pl.DeviceIdType.MESH
LANES = 128
f32 = jnp.float32
bf16 = jnp.bfloat16


def gll_tables():
    points = np.array([-1.0, -1.0 / math.sqrt(5.0), 1.0 / math.sqrt(5.0), 1.0])
    weights = np.array([1.0 / 6.0, 5.0 / 6.0, 5.0 / 6.0, 1.0 / 6.0])
    factor = np.array(
        [np.prod([points[j] - points[m] for m in range(4) if m != j]) for j in range(4)]
    )
    slopes = np.zeros((4, 4))
    for i in range(4):
        for j in range(4):
            if i != j:
                slopes[i, j] = factor[i] / (factor[j] * (points[i] - points[j]))
        slopes[i, i] = sum((1.0 / (points[i] - points[m]) for m in range(4) if m != i))
    return (slopes, weights)


SLOPES, WEIGHTS = gll_tables()


def combo(coefs, parts):
    total = None
    for c, v in zip(coefs, parts):
        if abs(c) < 1e-12:
            continue
        term = v * f32(c)
        total = term if total is None else total + term
    return total


def apply_line(table, v):
    phase = lax.broadcasted_iota(jnp.int32, (1, LANES), 1) % 4
    total = None
    for d in range(-3, 4):
        coef = jnp.zeros((1, LANES), f32)
        for p in range(4):
            if 0 <= p + d < 4 and abs(table[p, p + d]) > 1e-12:
                coef = jnp.where(phase == p, f32(table[p, p + d]), coef)
        moved = v if d == 0 else pltpu.roll(v, (LANES - d) % LANES, 1)
        total = coef * moved if total is None else total + coef * moved
    return total


def bands(flux):
    out = []
    for d in range(-3, 4):
        table = np.zeros((4, 4))
        for p in range(4):
            if 0 <= p + d < 4:
                table[p] = SLOPES[:, p] * SLOPES[:, p + d]
        out.append(apply_line(table, flux))
    return out


def stiff_line(band, v):
    total = band(3) * v
    for d in (-3, -2, -1, 1, 2, 3):
        total = total + band(3 + d) * pltpu.roll(v, (LANES - d) % LANES, 1)
    return total


def kernel(
    nc, ns, modes, groups,
    scale_hbm, forcing_ref, metric_ref, jac_ref, grad_hbm, div_hbm,
    v0, v1, v2, last, diag, coef, edge_row, edge_col,
    w, invp, mass, flux, zcat, gout, sums,
    row_e, col_e, row_d, col_d, row_m, row_i, col_m, col_i, row_fix, col_fix, row_k, col_k,
    row_c, col_c,
    row_tx, row_rx, col_tx, col_rx, cor_rx, ar_tx, ar_rx,
    source, factors, grad_ref, div_ref, scale_ref,
    htx_sem, hrx_sem, atx_sem, arx_sem, in_sem, table_sem,
):
    rows, cols = metric_ref.shape
    q = rows // 4
    n = nc * ns
    half = cols - LANES
    tiles = cols // LANES
    per = modes // groups
    slots = row_tx.shape[2]
    loads, sources = [], []
    for c in range(tiles):
        cut = pl.ds(c * LANES, LANES)
        loads += [
            pltpu.make_async_copy(jac_ref.at[:, cut], factors.at[0, c], in_sem.at[0, c]),
            pltpu.make_async_copy(metric_ref.at[:, cut], factors.at[1, c], in_sem.at[1, c]),
        ]
        sources.append(
            pltpu.make_async_copy(forcing_ref.at[:, :, cut], source.at[c], in_sem.at[2, c]))
    div_load = pltpu.make_async_copy(div_hbm, div_ref, table_sem.at[0])
    grad_load = pltpu.make_async_copy(grad_hbm, grad_ref, table_sem.at[1])
    scale_load = pltpu.make_async_copy(scale_hbm, scale_ref, table_sem.at[2])
    for copy in loads + sources + [scale_load]:
        copy.start()

    me_c, me_s = lax.axis_index("curve"), lax.axis_index("sub")
    me = me_c * ns + me_s
    up, down = lax.rem(me_c + nc - 1, nc), lax.rem(me_c + 1, nc)
    left, right = lax.rem(me_s + ns - 1, ns), lax.rem(me_s + 1, ns)

    def place(offset):
        target = lax.rem(me + offset, n)
        return (target // ns, lax.rem(target, ns))

    barrier = pltpu.get_barrier_semaphore()

    def greet(offset, carry):
        pl.semaphore_signal(barrier, inc=1, device_id=place(offset), device_id_type=MESH)
        return carry

    lax.fori_loop(1, n, greet, 0, unroll=True if n <= 32 else 1)

    def iota(shape, axis):
        return lax.broadcasted_iota(jnp.int32, shape, axis)

    def ways(shape):
        at = iota(shape, 1)
        return (at % 4 == 3) & (at != cols - 1), (at % 4 == 0) & (at != 0)

    lane_full = iota((q, cols), 1)
    lane = iota((q, LANES), 1)
    row_at = iota((q, cols), 0)
    edge_at = iota((q, LANES), 0)
    phase = lane_full % 4
    on_edge = (phase == 0) | (phase == 3)
    inside = (lane_full != 0) & (lane_full != cols - 1)

    def load(ref, m):
        return [ref[m, p * q:(p + 1) * q, :] for p in range(4)]

    def save(ref, m, parts):
        for p in range(4):
            ref[m, p * q:(p + 1) * q, :] = parts[p]

    def load2(ref):
        return [ref[p * q:(p + 1) * q, :] for p in range(4)]

    def join_cols(t, shape):
        take_next, take_prev = ways(shape)
        return t + jnp.where(
            take_next, pltpu.roll(t, cols - 1, 1),
            jnp.where(take_prev, pltpu.roll(t, 1, 1), 0.0))

    def join_rows(c):
        ph = lane % 4
        after = pltpu.roll(pltpu.roll(c, LANES - (LANES - 3), 1), q - 1, 0)
        before = pltpu.roll(pltpu.roll(c, LANES - 3, 1), 1, 0)
        return c + jnp.where((ph == 3) & (edge_at != q - 1), after,
                             jnp.where((ph == 0) & (edge_at != 0), before, 0.0))

    def pack(rows_ref, m, slot, h, tops):
        lo, hi = tops
        rows_ref[0, pl.ds(slot, 1), :] = h[0][0:1, :]
        rows_ref[1, pl.ds(slot, 1), :] = h[3][q - 1:q, :]
        save(w, m, joined(h))
        for p in range(4):
            at = 4 * slot + p
            lo = jnp.where(lane == at, pltpu.roll(h[p][:, :LANES], at, 1), lo)
            hi = jnp.where(lane == at, pltpu.roll(h[p][:, half:], at + 1, 1), hi)
        return lo, hi

    def halo_copies(k):
        plan = [
            (col_tx.at[k, 0, pl.ds(0, 1)], cor_rx.at[k, 3], (up, left)),
            (col_tx.at[k, 1, pl.ds(0, 1)], cor_rx.at[k, 2], (up, right)),
            (col_tx.at[k, 0, pl.ds(q - 1, 1)], cor_rx.at[k, 1], (down, left)),
            (col_tx.at[k, 1, pl.ds(q - 1, 1)], cor_rx.at[k, 0], (down, right)),
            (row_tx.at[k, 0], row_rx.at[k, 1], (up, me_s)),
            (row_tx.at[k, 1], row_rx.at[k, 0], (down, me_s)),
            (col_tx.at[k, 0], col_rx.at[k, 1], (me_c, left)),
            (col_tx.at[k, 1], col_rx.at[k, 0], (me_c, right)),
        ]
        return [
            pltpu.make_async_remote_copy(
                src_ref=src, dst_ref=dst, send_sem=htx_sem.at[k, e], recv_sem=hrx_sem.at[k, e],
                device_id=where, device_id_type=MESH)
            for e, (src, dst, where) in enumerate(plan)
        ]

    def send(k):
        for copy in halo_copies(k):
            copy.start()

    ends = ((0, 0), (q - 1, 3))
    tall = iota((slots, LANES), 0)
    wide_lane = iota((slots, LANES), 1)

    def to_rows(line, p0, target):
        found = jnp.where(wide_lane == 4 * tall + p0, line, 0.0)
        found = jnp.sum(found, axis=1, keepdims=True)
        return jnp.where(wide_lane == target, found, 0.0)

    def to_cols(block, p0, target):
        at = wide_lane == 4 * tall + p0
        spread = jnp.broadcast_to(block[:, target:target + 1], (slots, LANES))
        return jnp.sum(jnp.where(at, spread, 0.0), axis=0, keepdims=True)

    def at_sides(lo, hi):
        middle = [jnp.zeros((slots, LANES), f32)] * (tiles - 2)
        return jnp.concatenate([lo] + middle + [hi], axis=1)

    def side_tile(block, side):
        return block[:, half:] if side else block[:, :LANES]

    def arrive(k):
        for copy in halo_copies(k):
            copy.wait_recv()
        ph = iota((1, LANES), 1) % 4
        merged = []
        for side in range(2):
            above, below = cor_rx[k, side], cor_rx[k, 2 + side]
            above = jnp.where(ph == 0, pltpu.roll(above, LANES - 3, 1), 0.0)
            below = jnp.where(ph == 3, pltpu.roll(below, 3, 1), 0.0)
            c = col_rx[k, side]
            merged.append(
                c + jnp.where(edge_at == 0, above, 0.0) + jnp.where(edge_at == q - 1, below, 0.0))
        on_rows, on_cols = [], []
        for end, (at, p0) in enumerate(ends):
            t = join_cols(row_tx[k, end] + row_rx[k, end], (slots, cols))
            on_rows.append(t + at_sides(
                to_rows(merged[0][at:at + 1, :], p0, 0),
                to_rows(merged[1][at:at + 1, :], p0, LANES - 1)))
        for side in range(2):
            c = col_tx[k, side] + merged[side]
            for end, (at, p0) in enumerate(ends):
                line = to_cols(side_tile(row_rx[k, end], side), p0, (LANES - 1) * side)
                c = c + jnp.where(edge_at == at, line, 0.0)
            on_cols.append(c)
        return on_rows, on_cols

    def fixed(m):
        t = load(w, m)
        for p in range(4):
            pieces = [t[p][:, e * LANES:(e + 1) * LANES] for e in range(tiles)]
            for side, e in ((0, 0), (1, tiles - 1)):
                value = pltpu.roll(col_fix[side], LANES - 4 * m - p, 1)[:, 0:1]
                pieces[e] = pieces[e] + value * col_k[side, p]
            t[p] = jnp.concatenate(pieces, axis=1)
            blocks = [t[p][:8, :], t[p][8:q - 8, :], t[p][q - 8:, :]]
            for end, (at, p0) in enumerate(ends):
                line = row_fix[end, p, pl.ds(m, 1), :]
                spot = 7 * end if p != p0 else 1 + 5 * end
                blocks[2 * end] = blocks[2 * end] + jnp.where(row_at[:8, :] == spot, line, 0.0)
            t[p] = jnp.concatenate(blocks, axis=0)
        return t

    def joined(h):
        t0 = h[0] + jnp.where(row_at == 0, 0.0, pltpu.roll(h[3], 1, 0))
        t3 = h[3] + jnp.where(row_at == q - 1, 0.0, pltpu.roll(h[0], q - 1, 0))
        return [join_cols(t, (q, cols)) for t in (t0, h[1], h[2], t3)]

    def clear(parts):
        keep = [inside] * 4
        keep[0] = inside & (row_at != 0)
        keep[3] = inside & (row_at != q - 1)
        return [jnp.where(k, u, 0.0) for k, u in zip(keep, parts)]

    edge_w, mid_w = f32(1.0 / 6.0), f32(5.0 / 6.0)
    grid_lane = jnp.where(on_edge, edge_w, mid_w)
    mw, fw = [], []
    for copy in loads:
        copy.wait()
    for p in range(4):
        grid_w = grid_lane * (edge_w if p in (0, 3) else mid_w)
        mw.append(strided([factors.at[0, c] for c in range(tiles)], p, q) * grid_w)
        fw.append(strided([factors.at[1, c] for c in range(tiles)], p, q) * grid_w)
        mass[p * q:(p + 1) * q, :] = mw[p]
        flux[p * q:(p + 1) * q, :] = fw[p]
    zero = jnp.zeros((q, LANES), f32)
    tops = pack(row_tx.at[0], modes, modes, mw, (zero, zero))
    squared = SLOPES * SLOPES

    def per_line(fn, block):
        return jnp.concatenate(
            [fn(block[:, e * LANES:(e + 1) * LANES], e) for e in range(tiles)], axis=1)

    lap = [combo(squared[:, a], fw) + per_line(lambda v, e: apply_line(squared.T, v), fw[a])
           for a in range(4)]
    tops = pack(row_tx.at[0], modes + 1, modes + 1, lap, tops)
    for copy in sources:
        copy.wait()
    grad_load.start()
    div_load.start()

    def start_body(m, carry):
        h = [strided([source.at[c, m] for c in range(tiles)], p, q)
             * mass[p * q:(p + 1) * q, :] for p in range(4)]
        return pack(row_tx.at[0], m, m, h, carry)

    tops = lax.fori_loop(0, modes, start_body, tops, unroll=2)
    for side in range(2):
        col_tx[0, side] = join_rows(tops[side])
    pl.semaphore_wait(barrier, n - 1)
    send(0)
    scale_load.wait()

    basis = (v0, v1, v2)
    span = sums.shape[0] // SUMS
    scale_rows = jnp.zeros((slots, LANES), f32)
    scale_lanes = jnp.zeros((1, LANES), f32)
    lane_one = iota((1, LANES), 1)
    for m in range(modes):
        scale_rows = jnp.where(tall == m, scale_ref[m], scale_rows)
        scale_lanes = jnp.where(lane_one // 4 == m, scale_ref[m], scale_lanes)
    scale_rows = jnp.concatenate([scale_rows] * tiles, axis=1)
    coef[5] = scale_rows

    ffull, mfull = load2(flux), load2(mass)
    line_lane = iota((1, cols), 1)
    not_corner = (line_lane != 0) & (line_lane != cols - 1)
    for end, (at, p0) in enumerate(ends):
        cut = [f[at:at + 1, :] for f in ffull]
        pieces = [bands(cut[p0][:, e * LANES:(e + 1) * LANES]) for e in range(tiles)]
        for d in range(7):
            row_c[end, d:d + 1, :] = jnp.concatenate([b[d] for b in pieces], axis=1)
        row_c[end, 3:4, :] = row_c[end, 3:4, :] + jnp.where(
            not_corner, combo(SLOPES[:, p0] ** 2, cut), 0.0)
        row_c[end, 7:8, :] = mfull[p0][at:at + 1, :]
        for p in range(4):
            far = p if p != p0 else 3 - p0
            row_k[end, p:p + 1, :] = join_cols(
                combo(SLOPES[:, p0] * SLOPES[:, far], cut), (1, cols))
    for side in range(2):
        fc, mc, dc = zero, zero, zero
        reach = []
        for p in range(4):
            f = side_tile(ffull[p], side)
            base = half and (LANES - 4) * side
            cells = [jnp.broadcast_to(f[:, base + b:base + b + 1], (q, LANES)) for b in range(4)]
            b0 = 3 * side
            mass_cell = side_tile(mfull[p], side)[:, base + b0:base + b0 + 1]
            mine = lane % 4 == p
            fc = jnp.where(mine, cells[b0], fc)
            mc = jnp.where(mine, mass_cell, mc)
            dc = jnp.where(mine, combo(SLOPES[:, b0] ** 2, cells), dc)
            block = zero
            for b in range(4):
                if b != b0:
                    hit = lane == base + b
                    if b == 3 - b0:
                        hit = hit | (lane == base + b + 1 - 2 * side)
                    block = jnp.where(hit, combo(SLOPES[:, b0] * SLOPES[:, b], cells), block)
            reach.append(block)
        col_k[side, 0] = reach[0] + jnp.where(edge_at == 0, 0.0, pltpu.roll(reach[3], 1, 0))
        col_k[side, 1], col_k[side, 2] = reach[1], reach[2]
        col_k[side, 3] = reach[3] + jnp.where(
            edge_at == q - 1, 0.0, pltpu.roll(reach[0], q - 1, 0))
        for at, p0 in ends:
            dc = jnp.where((edge_at == at) & (lane % 4 == p0), 0.0, dc)
        for d, band in enumerate(bands(fc)):
            col_c[side, d] = band + dc if d == 3 else band
        col_c[side, 7] = mc

    def fill(b, slot, parts):
        v = jnp.concatenate(parts, axis=0)
        top = v.astype(bf16)
        at = pl.ds(pl.multiple_of(slot * rows, rows), rows)
        zcat[b, at, :cols] = top
        zcat[b, at, cols:] = (v - top.astype(f32)).astype(bf16)

    def multiply(b, table_ref):
        gout[b] = (
            jnp.dot(zcat[b], table_ref[:2 * cols, :], preferred_element_type=f32)
            + jnp.dot(zcat[b, :, :cols], table_ref[2 * cols:, :], preferred_element_type=f32))

    def build(it):
        tops = (zero, zero)
        for b in range(groups):
            base = b * per

            def first(slot, carry, b=b, base=base):
                m = base + slot
                t = load(w, m) if it == 0 else fixed(m)
                if it == 0:
                    inv = clear([1.0 / (u + scale_ref[m] * v)
                                 for u, v in zip(load(diag, 0), load(diag, 1))])
                    save(invp, m, inv)
                    zz = [u * v for u, v in zip(t, inv)]
                else:
                    zz = [u * v - f32(SIGMA) * o
                          for u, v, o in zip(t, load(invp, m), load(basis[it - 1], m))]
                save(basis[it], m, zz)
                fill(b, slot, zz)
                rz = [u * v for u, v in zip(t, zz)]
                rho = (rz[0] + rz[3]) * 0.5 + (rz[1] + rz[2])
                rho = jnp.where(on_edge, rho * 0.5, rho)
                sums[pl.ds(2 * it * span + m, 1), :] = jnp.sum(rho, axis=0, keepdims=True)
                f = load2(flux)
                fg = [f[a] * combo(SLOPES[a], zz) * scale_ref[m] for a in range(4)]
                ms = load2(mass)
                save(w, m, [ms[a] * zz[a] + combo(SLOPES[:, a], fg) for a in range(4)])
                return carry

            lax.fori_loop(0, per, first, 0, unroll=True)
            if it == 0 and b == 0:
                grad_load.wait()
                div_load.wait()
            multiply(b, grad_ref)

            def second(slot, carry, b=b, base=base):
                grad = gout[b, pl.ds(pl.multiple_of(slot * rows, rows), rows), :]
                fill(b, slot, [flux[...] * grad * scale_ref[base + slot]])
                return carry

            lax.fori_loop(0, per, second, 0, unroll=True)
            multiply(b, div_ref)

            def third(slot, carry, b=b, base=base):
                m = base + slot
                zz = load(basis[it], m)
                h = [u + gout[b, pl.ds(pl.multiple_of(slot * rows + p * q, q), q), :]
                     for p, u in enumerate(load(w, m))]
                zh = zz[0] * h[0] + zz[1] * h[1] + zz[2] * h[2] + zz[3] * h[3]
                sums[pl.ds((2 * it + 1) * span + m, 1), :] = jnp.sum(zh, axis=0, keepdims=True)
                return pack(row_e, m, m, h, carry)

            tops = lax.fori_loop(0, per, third, tops, unroll=True)
        col_e[0], col_e[1] = tops

    row_weight = jnp.where((line_lane % 4 == 0) | (line_lane % 4 == 3), 0.25, 0.5).astype(f32)
    corner = ((edge_at == 0) & (lane % 4 == 0)) | ((edge_at == q - 1) & (lane % 4 == 3))
    col_weight = jnp.where((lane % 4 == 0) | (lane % 4 == 3), 0.25, 0.5).astype(f32)
    col_weight = jnp.where(corner, 0.0, col_weight)
    own_slot = wide_lane // 4 == tall

    def fold(e, on_rows, on_cols):
        at = slice(e * span, e * span + slots)
        sums[at, :] = sums[at, :] + (on_rows[0] + on_rows[1])
        line = jnp.sum(on_cols[0] + on_cols[1], axis=0, keepdims=True)
        sums[at, :LANES] = sums[at, :LANES] + jnp.where(own_slot, line, 0.0)

    def step(it):
        on_rows, on_cols = arrive(it)
        row_now, col_now, row_s, col_s = [], [], [], []
        for i in range(2):
            if it == 0:
                t = on_rows[i]
                weight = t[modes:modes + 1, :] + scale_rows * t[modes + 1:modes + 2, :]
                row_m[i], row_i[i] = weight, 1.0 / weight
                c = on_cols[i]
                md, ld = zero, zero
                for p in range(4):
                    a, b = 4 * modes + p, 4 * modes + 4 + p
                    md = jnp.where(lane % 4 == p, c[:, a:a + 1], md)
                    ld = jnp.where(lane % 4 == p, c[:, b:b + 1], ld)
                weight = md + scale_lanes * ld
                col_m[i], col_i[i] = weight, 1.0 / weight
            r, c = on_rows[i] * row_i[i], on_cols[i] * col_i[i]
            if it > 0:
                r, c = r - f32(SIGMA) * row_d[it - 1, i], c - f32(SIGMA) * col_d[it - 1, i]
            row_d[it, i], col_d[it, i] = r, c
            row_now.append(r)
            col_now.append(c)
            row_s.append(per_line(
                lambda v, e, i=i: stiff_line(
                    lambda d: row_c[i, d:d + 1, e * LANES:(e + 1) * LANES], v), r))
            col_s.append(stiff_line(lambda d, i=i: col_c[i, d], c))
        row_out, col_out = [], []
        for end, (at, p0) in enumerate(ends):
            across = at_sides(
                to_rows(col_s[0][at:at + 1, :], p0, 0),
                to_rows(col_s[1][at:at + 1, :], p0, LANES - 1))
            r = row_now[end]
            row_out.append(
                row_e[end] + row_c[end, 7:8, :] * r + scale_rows * (row_s[end] + across))
        for side in range(2):
            total = col_s[side]
            for end, (at, p0) in enumerate(ends):
                line = to_cols(side_tile(row_s[end], side), p0, (LANES - 1) * side)
                total = total + jnp.where((edge_at == at) & (lane % 4 == p0), line, 0.0)
            col_out.append(
                col_e[side] + col_c[side, 7] * col_now[side] + scale_lanes * total)
        for i in range(2):
            row_tx[it + 1, i] = row_out[i]
            col_tx[it + 1, i] = join_rows(col_out[i])
        if it < ITERS - 1:
            send(it + 1)
        fold(2 * it,
             [row_weight * u * v for u, v in zip(row_now, on_rows)],
             [col_weight * u * v for u, v in zip(col_now, on_cols)])
        fold(2 * it + 1,
             [u * (a + b) for u, a, b in zip(row_now, [row_e[0], row_e[1]], row_out)],
             [jnp.where(corner, 0.0, u * (a + b))
              for u, a, b in zip(col_now, [col_e[0], col_e[1]], col_out)])
        lines.append(reduce_sums(it))
        if it == ITERS - 1:
            spread_sums()
            send(it + 1)
        for i, (at, p0) in enumerate(ends):
            col_fix[i] = scale_lanes * col_now[i]
            for p in range(4):
                row_fix[i, p] = scale_rows * row_now[i] * row_k[i, p:p + 1, :]

    wide = ar_tx.shape[1]
    gathered = ar_rx.at[pl.ds(1, n - 1)]
    lines = []

    def reduce_sums(it):
        base = 2 * it * span
        eye = iota((2 * span, wide), 0) + base == iota((2 * span, wide), 1)
        part = jnp.sum(sums[base:base + 2 * span, :], axis=1, keepdims=True)
        return jnp.sum(jnp.where(eye, part, 0.0), axis=0, keepdims=True)

    def spread_sums():
        line = sum(lines)
        ar_tx[...] = line
        ar_rx[0:1, :] = line

        def spread(i, carry):
            offset = jnp.where(i % 2 == 1, (i + 1) // 2, n - i // 2)
            pltpu.make_async_remote_copy(
                src_ref=ar_tx, dst_ref=ar_rx.at[pl.ds(offset, 1)],
                send_sem=atx_sem, recv_sem=arx_sem,
                device_id=place(offset), device_id_type=MESH).start()
            return carry

        lax.fori_loop(1, n, spread, 0, unroll=True if n <= 32 else 1)

    sums[...] = jnp.zeros_like(sums)
    for e in range(2):
        save(diag, e, load(w, modes + e))
    for it in range(ITERS):
        build(it)
        step(it)

    def finish(m, carry):
        save(last, m, clear(fixed(m)))
        return carry

    lax.fori_loop(0, modes, finish, 0, unroll=2)
    for k in range(ITERS):
        for copy in halo_copies(k):
            copy.wait_send()
    on_rows, on_cols = arrive(ITERS)
    pltpu.make_async_copy(gathered, gathered, arx_sem).wait()
    total = jnp.sum(ar_rx[...], axis=0, keepdims=True)
    solve(total, span, coef)
    on_lanes = [
        jnp.sum(jnp.where(own_slot, coef[e, :slots, :LANES], 0.0), axis=0, keepdims=True)
        for e in range(5)]
    for i in range(2):
        for ref, given, prior, weight, (c0, c1, c2, k0, k1) in (
                (edge_row, on_rows[i], row_d, row_m[i], [coef[e, :slots, :] for e in range(5)]),
                (edge_col, on_cols[i], col_d, col_m[i], on_lanes)):
            a, b, c = prior[0, i], prior[1, i], prior[2, i]
            ref[0, i] = c0 * a + c1 * b + c2 * c
            ref[1, i] = weight * (k0 * a - k1 * b - c1 * c) - c2 * given

    for copy in halo_copies(ITERS):
        copy.wait_send()
    pltpu.make_async_copy(gathered, gathered, atx_sem).wait()


def solve(total, span, coef):
    wide = total.shape[1]
    live = lax.broadcasted_iota(jnp.int32, (1, wide), 1) < coef.shape[1]
    b0, a0, b1, a1, b2, a2 = [
        jnp.where(live, total if e == 0 else pltpu.roll(total, wide - e * span, 1), 1.0)
        for e in range(SUMS)]
    sigma = f32(SIGMA)
    n1 = a0 - sigma * b0
    n2 = b1 - sigma * n1
    n3 = a1 - sigma * n2
    g02 = n3 + sigma * n2
    l1, l2 = b1 / a0, g02 / a0
    d1 = a1 - l1 * b1
    e12 = b2 - l1 * g02
    l3 = e12 / d1
    d2 = a2 - l2 * g02 - l3 * e12
    y1 = n1 - l1 * b0
    y2 = n2 - l2 * b0 - l3 * y1
    c2 = y2 / d2
    c1 = y1 / d1 - l3 * c2
    c0 = b0 / a0 - l1 * c1 - l2 * c2
    spot = (lax.broadcasted_iota(jnp.int32, (coef.shape[1], wide), 0)
            == lax.broadcasted_iota(jnp.int32, (coef.shape[1], wide), 1))
    for e, line in enumerate((c0, c1, c2, 1.0 - sigma * c0, c0 + sigma * c1)):
        tall = jnp.sum(jnp.where(spot, line, 0.0), axis=1, keepdims=True)
        coef[e] = jnp.broadcast_to(tall, coef.shape[1:])


def node_order(
    v0, v1, v2, last, diag, coef, edge_row, edge_col, sol_ref, res_ref,
    sol_buf, res_buf, sem,
):
    modes, rows, cols = v0.shape
    q, tiles = rows // 4, cols // LANES

    lane = lax.broadcasted_iota(jnp.int32, (q, LANES), 1)

    def stores(m):
        return [
            pltpu.make_async_copy(
                buf.at[c, m], out.at[m, :, pl.ds(c * LANES, LANES)], sem.at[k, c, m])
            for k, (buf, out) in enumerate(((sol_buf, sol_ref), (res_buf, res_ref)))
            for c in range(tiles)
        ]

    def body(m, carry):
        c0, c1, c2, k0, k1, scale = [coef[e, pl.ds(m, 1), :] for e in range(6)]
        for p in range(4):
            cut = slice(p * q, (p + 1) * q)
            a, b, c = v0[m, cut, :], v1[m, cut, :], v2[m, cut, :]
            x = c0 * a + c1 * b + c2 * c
            weight = diag[0, cut, :] + scale * diag[1, cut, :]
            r = weight * (k0 * a - k1 * b - c1 * c) - c2 * last[m, cut, :]
            for field, (buf, whole) in enumerate(((sol_buf, x), (res_buf, r))):
                for t in range(tiles):
                    piece = whole[:, t * LANES:(t + 1) * LANES]
                    for side, own in ((0, 0), (1, tiles - 1)):
                        if t == own:
                            spot = (LANES - 1) * side
                            line = pltpu.roll(
                                edge_col[field, side], spot + LANES - 4 * m - p, 1)
                            piece = piece + jnp.where(lane == spot, line, 0.0)
                    buf[t, m, pl.ds(p, q, stride=4), :] = piece
        for field, buf in enumerate((sol_buf, res_buf)):
            for end, at in ((0, 0), (1, rows - 1)):
                line = edge_row[field, end, pl.ds(m, 1), :]
                for t in range(tiles):
                    buf[t, m, at:at + 1, :] = line[:, t * LANES:(t + 1) * LANES]
        for copy in stores(m):
            copy.start()
        return carry

    lax.fori_loop(0, modes, body, 0, unroll=OUT_UNROLL)

    def drain(m, carry):
        for copy in stores(m):
            copy.wait()
        return carry

    lax.fori_loop(0, modes, drain, 0)


def strided(refs, p, q):
    return jnp.concatenate([ref[pl.ds(p, q, stride=4), :] for ref in refs], axis=1)


def stack_table(table):
    top = table.astype(bf16)
    low = (table - top.astype(np.float32)).astype(bf16)
    return np.concatenate([top, top, low], axis=0)


def shards(nc, ns, forcing, metric, jacobian, mode_scale):
    modes, rows, cols = forcing.shape
    block = np.kron(np.eye(cols // 4), SLOPES).astype(np.float32)
    grad, div = stack_table(block.T), stack_table(block)
    n, q, tiles = nc * ns, rows // 4, cols // LANES
    groups = GROUPS if modes % GROUPS == 0 else 1
    per = modes // groups
    slots = -(-(modes + 2) // 8) * 8
    vm = pl.BlockSpec(memory_space=pltpu.VMEM)
    hbm = pl.BlockSpec(memory_space=pltpu.HBM)
    rounds = ITERS + 1
    span = slots
    wide = -(-SUMS * span // LANES) * LANES
    field = pltpu.VMEM((modes, rows, cols), f32)
    split = pltpu.VMEM((tiles, modes, rows, LANES), f32)
    table = pltpu.VMEM(grad.shape, bf16)
    shape = jax.ShapeDtypeStruct(forcing.shape, f32)

    def on_rows(*lead):
        return pltpu.VMEM((*lead, slots, cols), f32)

    def on_cols(*lead):
        return pltpu.VMEM((*lead, q, LANES), f32)

    built = pl.pallas_call(
        functools.partial(kernel, nc, ns, modes, groups),
        out_shape=[shape] * 4 + [
            jax.ShapeDtypeStruct((2, rows, cols), f32),
            jax.ShapeDtypeStruct((6, span, cols), f32),
            jax.ShapeDtypeStruct((2, 2, slots, cols), f32),
            jax.ShapeDtypeStruct((2, 2, q, LANES), f32)],
        in_specs=[hbm] * 6,
        out_specs=[vm] * 8,
        scratch_shapes=[
            pltpu.VMEM((modes + 2, rows, cols), f32),
            field,
            pltpu.VMEM((rows, cols), f32),
            pltpu.VMEM((rows, cols), f32),
            pltpu.VMEM((groups, per * rows, 2 * cols), bf16),
            pltpu.VMEM((groups, per * rows, cols), f32),
            pltpu.VMEM((SUMS * span, cols), f32),
            on_rows(2), on_cols(2),
            on_rows(ITERS, 2), on_cols(ITERS, 2),
            on_rows(2), on_rows(2), on_cols(2), on_cols(2),
            on_rows(2, 4), on_cols(2),
            pltpu.VMEM((2, 8, cols), f32),
            on_cols(2, 4),
            pltpu.VMEM((2, 8, cols), f32),
            on_cols(2, 8),
            on_rows(rounds, 2), on_rows(rounds, 2),
            on_cols(rounds, 2), on_cols(rounds, 2),
            pltpu.VMEM((rounds, 4, 1, LANES), f32),
            pltpu.VMEM((1, wide), f32),
            pltpu.VMEM((n, wide), f32),
            split,
            pltpu.VMEM((2, tiles, rows, LANES), f32),
            table, table,
            pltpu.SMEM((modes,), f32),
            pltpu.SemaphoreType.DMA((rounds, 8)),
            pltpu.SemaphoreType.DMA((rounds, 8)),
            pltpu.SemaphoreType.DMA,
            pltpu.SemaphoreType.DMA,
            pltpu.SemaphoreType.DMA((3, tiles)),
            pltpu.SemaphoreType.DMA((3,)),
        ],
        compiler_params=pltpu.CompilerParams(
            collective_id=0, has_side_effects=True, vmem_limit_bytes=41943040),
    )(*[pltpu.with_memory_space_constraint(v, pltpu.HBM) for v in (mode_scale, forcing, metric, jacobian, jnp.asarray(grad), jnp.asarray(div))])
    return pl.pallas_call(
        node_order,
        out_shape=[shape] * 2,
        in_specs=[vm] * 8,
        out_specs=[hbm, hbm],
        scratch_shapes=[
            split, split, pltpu.SemaphoreType.DMA((2, tiles, modes))],
        compiler_params=pltpu.CompilerParams(vmem_limit_bytes=16 * 1024 * 1024),
    )(*built)


def solution(mesh):
    placed = (P(None, "curve", "sub"), P("curve", "sub"), P("curve", "sub"), P())
    return jax.shard_map(
        functools.partial(shards, mesh.shape["curve"], mesh.shape["sub"]),
        mesh=mesh,
        in_specs=placed,
        out_specs=(P(None, "curve", "sub"), P(None, "curve", "sub")),
        check_vma=False,
    )
```
